32 devices in a mesh: ctx: 4 (over z), grp: 8 (over y, x, core).
Axes of the slice: x: 2, y: 2, z: 4, core: 2. Of those that a mesh axis runs over, the one named last changes fastest.
Arguments:
- latent: bfloat16 [8, 512, 576], P('grp', 'ctx'), may hold values from -6 to 6
- queries: bfloat16 [8, 16, 73728], P('grp', 'ctx'), may hold values from -4 to 4
- out_grad: bfloat16 [8, 16, 65536], P('grp', 'ctx'), may hold values from -6 to 6
- hidden: bfloat16 [8, 512, 7168], P('grp', None, 'ctx'), may hold values from -6 to 6
- doc_ids: int32 [8, 512], P('grp', 'ctx'), may hold values from 0 to 7, never falling along the last dimension, each value on 1 to 256 neighbouring positions
- clip_limits: float32 [8, 8], P('grp'), may hold values from 0.05 to 20
Outputs:
- grad_keys: bfloat16 [8, 512, 576], P('grp', 'ctx')
- weight_grad: float32 [576, 7168], P('grp', 'ctx')
The draws below stay inside these ranges and needn't reach their ends.
Inputs may be any that keep to these rules, and one draw needn't show every extreme that they name: `doc_ids`: within each group the ids never fall; each document has 1 to 256 tokens and one has exactly 256.
All inputs are finite; a program needn't handle non-finite values.
Results may differ from the reference program's by a relative error of at most 0.0095.
Values may be sent and summed in bfloat16 or wider, within the bound.
A program may use at most 64 MiB of HBM per device.

```python
import math
import jax
import jax.numpy as jnp
import numpy as np
from jax import lax

D = 7168
LATENT = 512
HEADS = 128
KW = 576
TOK_DEV = 128
Q_DEV = 4
NDOC = 8
SEQ = 512
MOST = 256
WIN = 260
QROWS = 16
GROUPS = 8
N_CTX = 4


def plant_plan(key):
    shards = SEQ // TOK_DEV
    half = KW // 2
    group_keys = jax.random.split(jax.random.fold_in(key, 101), GROUPS)
    orders = jax.vmap(lambda one: jax.random.permutation(one, KW))(group_keys)
    ranks = jnp.argsort(orders, axis=1)
    chosen = ranks < half
    flips = jax.random.bernoulli(jax.random.fold_in(key, 102), 0.5, (GROUPS, shards, KW))
    signs = jnp.where(flips, 1.0, -1.0).astype(jnp.float32)
    strength = 2.5 + 0.5 * jax.random.randint(jax.random.fold_in(key, 103), (GROUPS, shards), 0, 4).astype(jnp.float32)
    head_pick = jax.random.randint(jax.random.fold_in(key, 104), (GROUPS, shards), 0, HEADS)
    return (chosen, signs, strength, head_pick)


def draw_latent(key, part):
    chosen, signs, strength, head_pick = plant_plan(key)
    shards = SEQ // TOK_DEV
    base_key = jax.random.fold_in(key, 201)
    base = jnp.clip(jax.random.normal(base_key, (GROUPS, SEQ, KW), jnp.float32), -6.0, 6.0)
    base = base.reshape(GROUPS, shards, TOK_DEV, KW)
    slot = jnp.arange(TOK_DEV)[None, None, :, None]
    magnitude = jnp.where(slot == TOK_DEV - 1, 5.0, 4.96875).astype(jnp.float32)
    planted = magnitude * signs[:, :, None, :]
    placed = (slot >= TOK_DEV - 2) & chosen[:, None, None, :]
    result = jnp.where(placed, planted, base)
    return result.reshape(GROUPS, SEQ, KW).astype(jnp.bfloat16)


def draw_queries(key, part):
    chosen, signs, strength, head_pick = plant_plan(key)
    shards = SEQ // TOK_DEV
    rows_dev = QROWS // shards
    base_key = jax.random.fold_in(key, 301)
    base = jnp.clip(0.5 * jax.random.normal(base_key, (GROUPS, QROWS, HEADS * KW), jnp.float32), -4.0, 4.0)
    base = base.reshape(GROUPS, shards, rows_dev, HEADS, KW)
    target = strength[:, :, None] * signs * chosen[:, None, :].astype(jnp.float32)
    last_row = (jnp.arange(rows_dev) == rows_dev - 1)[None, None, :, None, None]
    head_hit = (jnp.arange(HEADS)[None, None, :] == head_pick[:, :, None])[:, :, None, :, None]
    result = jnp.where(last_row & head_hit, target[:, :, None, None, :], base)
    return result.reshape(GROUPS, QROWS, HEADS * KW).astype(jnp.bfloat16)


def block_levels(stream_key, extent, cuts, smallest, high):
    def one(dim, blocks):
        steps = jax.random.uniform(jax.random.fold_in(jax.random.fold_in(stream_key, 6), dim), (blocks,), jnp.float32, smallest / len(cuts), high / len(cuts))
        return jnp.repeat(jnp.exp(steps), extent[dim] // blocks).reshape((-1,) + (1,) * (len(extent) - dim - 1))

    gain = one(*cuts[0])
    for cut in cuts[1:]:
        gain = gain * one(*cut)
    return gain


def length_profile(count, total, bound, skew):
    portions = [(1 << 20) // math.isqrt(standing ** skew) + 1 for standing in range(2, count + 1)]
    spare, counts = total - bound - (count - 1), [1] * (count - 1)
    while spare > 0:
        movable = [i for i in range(count - 1) if counts[i] < bound]
        whole, remaining = sum([portions[i] for i in movable]), spare
        for i in movable:
            addition = min(bound - counts[i], max(1, remaining * portions[i] // whole), spare)
            counts[i] = counts[i] + addition
            spare = spare - addition
    return np.array([bound] + counts)


def uneven_parts(own_key, number_of, total, limit, slope):
    if number_of == 2:
        one = jax.random.randint(own_key, (), max(1, total - limit), min(limit, total - 1) + 1)
        return jnp.stack([one, total - one])
    sizes = jnp.asarray(length_profile(number_of, total, limit, slope), jnp.int32)
    pairs = (number_of - 1) // 2
    donor, sink = sizes[1:1 + 2 * pairs:2], sizes[2:2 + 2 * pairs:2]
    slack = jnp.minimum(donor - 1, limit - sink)
    passed = jax.random.randint(jax.random.fold_in(own_key, 1), (pairs,), 0, 1 << 20) % (slack + 1)
    sizes = sizes.at[1:1 + 2 * pairs:2].set(donor - passed).at[2:2 + 2 * pairs:2].set(sink + passed)
    return sizes[jax.random.permutation(jax.random.fold_in(own_key, 2), number_of)]


def normal_values(key, extent, width, most, cuts=(), kind=jnp.bfloat16):
    values = jax.random.normal(key, extent, jnp.float32) * width
    if len(cuts) > 0:
        values = block_levels(key, extent, cuts, -0.22, 0.18) * values
    return jnp.clip(values, min=-most, max=most).astype(kind)


def setup_inputs(seed: int = 0) -> dict:
    streams_of = jax.random.split(jax.random.key(seed), 7)
    return {
        "latent": draw_latent(jax.random.fold_in(streams_of[6], 71), 0),
        "queries": draw_queries(jax.random.fold_in(streams_of[6], 71), 0),
        "out_grad": normal_values(streams_of[2], (GROUPS, QROWS, HEADS * LATENT), 1.0, 6.0, ((0, 8), (1, 4))),
        "hidden": normal_values(streams_of[3], (GROUPS, SEQ, D), 1.0, 6.0, ((0, 8), (2, 4))),
        "doc_ids": jax.vmap(lambda own: jnp.searchsorted(jnp.cumsum(uneven_parts(own, NDOC, SEQ, MOST, 2)), jnp.arange(SEQ), side="right"))(jax.random.split(streams_of[4], GROUPS)).reshape((GROUPS, SEQ)).astype(jnp.int32),
        "clip_limits": jnp.clip(jnp.exp(math.log(20.0) - 5.9914645 * jax.random.uniform(streams_of[5], (GROUPS, NDOC), jnp.float32) ** block_levels(streams_of[5], (GROUPS, NDOC), ((0, 8),), -0.2, 0.2)), 0.05, 20.0),
    }


score_scale = 192.0 ** (-0.5)
norm_eps = 1e-06

def device_part(latent_g, queries_g, grads_g, ids_g, index):
    first_query = (index * TOK_DEV + TOK_DEV - Q_DEV).astype(jnp.int32)
    start = jnp.clip(first_query + Q_DEV - WIN, 0, SEQ - WIN).astype(jnp.int32)
    query_block = lax.dynamic_slice_in_dim(queries_g, (index * Q_DEV).astype(jnp.int32), Q_DEV, 0)
    query_block = query_block.reshape(Q_DEV, HEADS, KW).astype(jnp.float32)
    grad_block = lax.dynamic_slice_in_dim(grads_g, (index * Q_DEV).astype(jnp.int32), Q_DEV, 0)
    grad_block = grad_block.reshape(Q_DEV, HEADS, LATENT).astype(jnp.float32)
    window_keys = lax.dynamic_slice_in_dim(latent_g, start, WIN, 0).astype(jnp.float32)
    window_ids = lax.dynamic_slice_in_dim(ids_g, start, WIN, 0)
    key_pos = start + jnp.arange(WIN, dtype=jnp.int32)
    query_pos = first_query + jnp.arange(Q_DEV, dtype=jnp.int32)
    query_ids = lax.dynamic_slice_in_dim(ids_g, first_query, Q_DEV, 0)
    allowed = (window_ids[None, :] == query_ids[:, None]) & (key_pos[None, :] <= query_pos[:, None])
    scores = jnp.einsum('qhc,kc->qhk', query_block, window_keys) * score_scale
    scores = jnp.where(allowed[:, None, :], scores, -1e+30)
    top_score = lax.optimization_barrier(jnp.max(scores, axis=-1, keepdims=True))
    weights = jnp.exp(scores - top_score)
    weights = weights / lax.optimization_barrier(jnp.sum(weights, axis=-1, keepdims=True))
    prob_grad = jnp.einsum('qhc,kc->qhk', grad_block, window_keys[:, :LATENT])
    row_dots = lax.optimization_barrier(jnp.sum(weights * prob_grad, axis=-1, keepdims=True))
    score_grad = (weights * (prob_grad - row_dots) * score_scale).astype(jnp.bfloat16).astype(jnp.float32)
    weights_low = weights.astype(jnp.bfloat16).astype(jnp.float32)
    key_grad = jnp.einsum('qhk,qhc->kc', score_grad, query_block)
    value_grad = jnp.einsum('qhk,qhc->kc', weights_low, grad_block)
    key_grad = key_grad.at[:, :LATENT].add(value_grad)
    full = lax.dynamic_update_slice(jnp.zeros((SEQ, KW), jnp.float32), key_grad, (start, jnp.int32(0)))
    return full.astype(jnp.bfloat16)

def reference(latent, queries, out_grad, hidden, doc_ids, clip_limits):

    def per_group(total, group):
        latent_g, queries_g, grads_g, hidden_g, ids_g, limits_g = group
        parts = lax.map(lambda index: device_part(latent_g, queries_g, grads_g, ids_g, index), jnp.arange(N_CTX, dtype=jnp.int32))
        grad_keys = lax.optimization_barrier(jnp.sum(parts.astype(jnp.float32), axis=0)).astype(jnp.bfloat16)
        values = grad_keys.astype(jnp.float32)
        member = (ids_g[:, None] == jnp.arange(NDOC, dtype=jnp.int32)[None, :]).astype(jnp.float32)
        norms = lax.optimization_barrier(jnp.sum(member * lax.optimization_barrier(jnp.sum(values * values, axis=1))[:, None], axis=0))
        factor = jnp.minimum(1.0, limits_g / jnp.sqrt(norms + norm_eps))
        scaled = (values * lax.optimization_barrier(jnp.sum(member * factor[None, :], axis=1))[:, None]).astype(jnp.bfloat16)
        term = jnp.dot(scaled.T, hidden_g, preferred_element_type=jnp.float32)
        return (total + term, grad_keys)
    weight_grad, grad_keys = lax.scan(per_group, jnp.zeros((KW, D), jnp.float32), (latent, queries, out_grad, hidden, doc_ids, clip_limits))
    return (grad_keys, weight_grad)
```

```python
import functools
import math

import jax
import jax.numpy as jnp
from jax import lax
from jax.experimental import pallas as pl
from jax.experimental.pallas import tpu as pltpu
from jax.sharding import PartitionSpec as P

LATENT = 512
HEADS = 128


score_scale = 192.0 ** (-0.5)
norm_eps = 1e-06

BF = jnp.bfloat16
F32 = jnp.float32


def dot(a, b, dims):
    return lax.dot_general(a, b, (dims, ((), ())), preferred_element_type=F32)


def col_chunks(cols):
    half = cols // 2
    first = -(-(half // 2) // 128) * 128
    out = []
    for start, width in ((0, first), (first, half - first)):
        for path in (0, 1):
            out.append((path * half + start, width, path))
    return out


def body(cfg, *refs):
    n = cfg["n"]
    tok = cfg["tok"]
    kw = cfg["kw"]
    qd = cfg["qd"]
    reach = cfg["reach"]
    rows_of = cfg["rows_of"]
    span = cfg["span"]
    ndocs = cfg["ndocs"]
    pieces = cfg["pieces"]
    scatter = cfg["scatter"]
    (lat_t, ids, lim, q_hbm, g_hbm, h_hbm, gk_out, w_out) = refs[:8]
    (qraw, graw, hid, qs, gs, kbuf, idbuf, psend, precv, full, scT, local_sem, key_s, key_r,
     id_s, id_r, part_s, part_r, up_s, up_r, dn_s, dn_r, lat) = refs[8:31]
    tail = refs[31:]
    d = lax.axis_index("ctx")
    m = lax.axis_index("grp")
    wide = -(-kw // 128) * 128
    pad = wide - kw
    pair = 2 * kw

    copy_q = pltpu.make_async_copy(q_hbm, qraw, local_sem.at[0])
    copy_g = pltpu.make_async_copy(g_hbm, graw, local_sem.at[1])
    copy_h = pltpu.make_async_copy(h_hbm, hid, local_sem.at[2])
    copy_q.start()
    copy_g.start()
    copy_h.start()

    def remote(src, dst, ss, rs, **where):
        axis, index = next(iter(where.items()))
        return pltpu.make_async_remote_copy(
            src_ref=src, dst_ref=dst, send_sem=ss, recv_sem=rs,
            device_id={axis: index}, device_id_type=pl.DeviceIdType.MESH,
        )

    barrier = pltpu.get_barrier_semaphore()
    for o in range(1, n):
        pl.semaphore_signal(barrier, inc=1, device_id={"ctx": lax.rem(d + o, n)},
                            device_id_type=pl.DeviceIdType.MESH)
    flips = []
    if scatter:
        bits = [lax.rem(m, 2), lax.rem(m // 2, 2), lax.rem(m // 4, 2)]
        flips = [m + (1 - 2 * bits[i]) * (1 << i) for i in range(3)]
        for f in flips:
            pl.semaphore_signal(barrier, inc=1, device_id={"grp": f},
                                device_id_type=pl.DeviceIdType.MESH)
    keys_t = jnp.concatenate([lat_t[0].astype(F32), jnp.zeros((pad, tok), F32)], axis=0)
    lat[0] = jnp.transpose(keys_t)[:, :kw].astype(BF)
    pl.semaphore_wait(barrier, n - 1 + len(flips))

    def key_copy(k):
        r = rows_of[k]
        return remote(lat.at[0, pl.ds(tok - r, r)], kbuf.at[k - 1, pl.ds(0, r)],
                      key_s.at[k - 1], key_r.at[k - 1], ctx=lax.rem(d + k, n))

    def id_copy(o):
        return remote(ids, idbuf.at[d], id_s.at[o - 1], id_r.at[o - 1], ctx=lax.rem(d + o, n))

    for k in range(1, reach):
        @pl.when(d + k < n)
        def _(k=k):
            key_copy(k).start()

    for o in range(1, n):
        id_copy(o).start()
    for k in range(1, reach):
        @pl.when(d - k < 0)
        def _(k=k):
            kbuf[k - 1] = jnp.zeros_like(kbuf[k - 1])
    idbuf[d] = ids[...]

    def repack(src, dst, width):
        group = 16 // qd

        def step(i, _):
            got = [
                src[0, :, pl.ds(pl.multiple_of((i * group + t) * width, 128), width)].astype(F32)
                for t in range(group)
            ]
            dst[pl.ds(pl.multiple_of(i * 16, 16), 16), :] = jnp.concatenate(got, axis=0).astype(BF)
            return 0

        lax.fori_loop(0, (HEADS // 2) // group, step, 0)

    copy_q.wait()
    repack(qraw, qs, pair)
    copy_g.wait()
    repack(graw, gs, 2 * LATENT)

    R = (HEADS // 2) * qd
    qrow = lax.broadcasted_iota(jnp.int32, (R, 1), 0) % qd
    own_ids = ids[...]
    qid = jnp.zeros((R, 1), jnp.int32)
    for i in range(qd):
        qid = jnp.where(qrow == i, own_ids[:, tok - qd + i:tok - qd + i + 1], qid)

    def query(par):
        return qs[:, 0:wide] if par == 0 else qs[:, pair - wide:pair]

    def grad(par):
        return gs[:, par * LATENT:(par + 1) * LATENT]

    def keys_of(k):
        return lat[0] if k == 0 else kbuf[k - 1, 0:rows_of[k], :]

    def block_products(k):
        kb = keys_of(k)
        zero = jnp.zeros((rows_of[k], pad), BF)
        padded = [jnp.concatenate([kb, zero], axis=1), jnp.concatenate([zero, kb], axis=1)]
        s = [dot(query(par), padded[par], ((1,), (1,))) for par in (0, 1)]
        dp = [dot(grad(par), kb[:, :LATENT], ((1,), (1,))) for par in (0, 1)]
        return s, dp

    products = [block_products(0)]

    for o in range(1, n):
        id_copy(o).wait_send()
        remote(ids, idbuf.at[lax.rem(d - o + n, n)], id_s.at[o - 1], id_r.at[o - 1],
               ctx=lax.rem(d + o, n)).wait_recv()
    for k in range(1, reach):
        @pl.when(d - k >= 0)
        def _(k=k):
            key_copy(k).wait_recv()
    for k in range(1, reach):
        products.append(block_products(k))

    allowed = []
    for k in range(reach):
        r = rows_of[k]
        row = own_ids if k == 0 else idbuf[jnp.maximum(d - k, 0)]
        row = row[:, tok - r:]
        lane = lax.broadcasted_iota(jnp.int32, (1, r), 1)
        ok = qid == row
        if k == 0:
            ok = ok & (lane <= tok - qd + qrow)
        else:
            reachable = jnp.where(lane + (tok - r) >= (k + 1) * tok - span, 1, 0)
            reachable = reachable * jnp.where(d - k >= 0, 1, 0)
            ok = ok & (reachable == 1)
        allowed.append(ok)

    dscores, probs = [[], []], [[], []]
    for par in (0, 1):
        s = [jnp.where(allowed[k], products[k][0][par] * score_scale, -1e30) for k in range(reach)]
        top = functools.reduce(jnp.maximum, [jnp.max(x, axis=1, keepdims=True) for x in s])
        w = [jnp.exp(x - top) for x in s]
        total = sum(jnp.sum(x, axis=1, keepdims=True) for x in w)
        w = [x / total for x in w]
        dps = [products[k][1][par] for k in range(reach)]
        rd = sum(jnp.sum(a * b, axis=1, keepdims=True) for a, b in zip(w, dps))
        for k in range(reach):
            dscores[par].append((w[k] * (dps[k] - rd) * score_scale).astype(BF))
            probs[par].append(w[k].astype(BF))

    def part_of(k):
        a = dot(dscores[0][k], query(0), ((0,), (0,)))[:, :kw]
        b = dot(dscores[1][k], query(1), ((0,), (0,)))[:, pad:pad + kw]
        v = dot(probs[0][k], grad(0), ((0,), (0,))) + dot(probs[1][k], grad(1), ((0,), (0,)))
        return (a + b + jnp.concatenate([v, jnp.zeros((rows_of[k], kw - LATENT), F32)], axis=1)).astype(BF)

    def part_copy(k, to):
        r = rows_of[k]
        return remote(psend.at[k - 1, pl.ds(0, r)], precv.at[k - 1, pl.ds(0, r)],
                      part_s.at[k - 1], part_r.at[k - 1], ctx=to)

    for k in range(1, reach):
        psend[k - 1, 0:rows_of[k], :] = part_of(k)

        @pl.when(d - k >= 0)
        def _(k=k):
            part_copy(k, jnp.maximum(d - k, 0)).start()

        @pl.when(d + k >= n)
        def _(k=k):
            precv[k - 1] = jnp.zeros_like(precv[k - 1])
    mine = part_of(0).astype(F32)

    eye = lax.broadcasted_iota(jnp.int32, (tok, tok), 0) == lax.broadcasted_iota(jnp.int32, (tok, tok), 1)
    doc_lane = lax.broadcasted_iota(jnp.int32, (1, 128), 1)
    member = []
    for j in range(n):
        col = jnp.sum(jnp.where(eye, idbuf[j], 0).astype(F32), axis=1, keepdims=True)
        member.append(jnp.where(col == doc_lane.astype(F32), 1.0, 0.0))

    for k in range(1, reach):
        @pl.when(d + k < n)
        def _(k=k):
            part_copy(k, jnp.maximum(d - k, 0)).wait_recv()
    for k in range(1, reach):
        r = rows_of[k]
        got = precv[k - 1, 0:r, :].astype(F32)
        if r < tok:
            got = jnp.concatenate([jnp.zeros((tok - r, kw), F32), got], axis=0)
        mine = mine + got
    mine_low = mine.astype(BF)
    full[d] = mine_low

    piece = tok // pieces

    def relay(direction, s, p):
        ss, rs = (up_s, up_r) if direction > 0 else (dn_s, dn_r)
        block = jnp.clip(d - direction * s, 0, n - 1)
        ref = full.at[block, pl.ds(p * piece, piece)]
        return remote(ref, ref, ss.at[s, p], rs.at[s, p], ctx=jnp.clip(d + direction, 0, n - 1))

    def arriving(direction, s, p):
        ss, rs = (up_s, up_r) if direction > 0 else (dn_s, dn_r)
        block = jnp.clip(d - direction * (s + 1), 0, n - 1)
        ref = full.at[block, pl.ds(p * piece, piece)]
        return remote(ref, ref, ss.at[s, p], rs.at[s, p], ctx=jnp.clip(d + direction, 0, n - 1))

    def can_send(direction, s):
        if direction > 0:
            return (d - s >= 0) & (d + 1 < n)
        return (d + s < n) & (d - 1 >= 0)

    def will_get(direction, s):
        return d - s - 1 >= 0 if direction > 0 else d + s + 1 < n

    for p in range(pieces):
        for direction in (1, -1):
            @pl.when(can_send(direction, 0))
            def _(p=p, direction=direction):
                relay(direction, 0, p).start()
    padded_out = jnp.concatenate([mine_low.astype(F32), jnp.zeros((tok, pad), F32)], axis=1)
    gk_out[0] = jnp.transpose(padded_out)[:kw].astype(BF)
    for s in range(n - 1):
        for p in range(pieces):
            for direction in (1, -1):
                @pl.when(will_get(direction, s))
                def _(p=p, s=s, direction=direction):
                    arriving(direction, s, p).wait_recv()
                if s + 1 < n - 1:
                    @pl.when(can_send(direction, s + 1))
                    def _(p=p, s=s, direction=direction):
                        relay(direction, s + 1, p).start()

    norms = jnp.zeros((1, 128), F32)
    for j in range(n):
        v = full[j].astype(F32)
        norms = norms + jnp.sum(member[j] * jnp.sum(v * v, axis=1, keepdims=True), axis=0, keepdims=True)
    limits = lim[...]
    if ndocs < 128:
        limits = jnp.concatenate([limits, jnp.zeros((1, 128 - ndocs), F32)], axis=1)
    factor = jnp.minimum(1.0, limits / jnp.sqrt(norms + norm_eps))
    share = kw // 8
    for j in range(n):
        f = jnp.sum(member[j] * factor, axis=1, keepdims=True)
        scaled = (full[j].astype(F32) * f).astype(BF).astype(F32)
        scaled = jnp.concatenate([scaled, jnp.zeros((tok, pad), F32)], axis=1)
        turned = jnp.transpose(scaled)
        if scatter:
            for b in range(8):
                scT[b % 2, (b // 2) * share:(b // 2 + 1) * share, j * tok:(j + 1) * tok] = (
                    turned[b * share:(b + 1) * share].astype(BF))
        else:
            scT[:, j * tok:(j + 1) * tok] = turned[:kw].astype(BF)

    copy_h.wait()
    if not scatter:
        w_out[...] = dot(scT[...], hid[0], ((1,), (0,)))
    else:
        chunks = col_chunks(w_out.shape[1])
        nc = len(chunks)
        bufs = [tail[7 * i:7 * i + 7] for i in range(nc)]
        rs_s, rs_r = tail[7 * nc:]
        core, xb, yb = bits

        def hop(i, stage):
            path = chunks[i][2]
            bit = 0 if stage == 0 else ((1, 2) if path == 0 else (2, 1))[stage - 1]
            s1, r1, acc, s2, r2, s3, r3 = bufs[i]
            src, dst = ((s1, r1), (s2, r2), (s3, r3))[stage]
            return remote(src, dst, rs_s.at[i, stage], rs_r.at[i, stage], grp=flips[bit])

        def block(path, moving, other):
            return other * 2 + moving if path == 0 else moving * 2 + other

        def product(i, half):
            start, width, _ = chunks[i]
            return dot(scT[half], hid[0, :, start:start + width], ((1,), (0,)))

        def send_first(i):
            bufs[i][0][...] = product(i, 1 - core).astype(BF)
            hop(i, 0).start()

        def own(i):
            bufs[i][2][...] = product(i, core).reshape(bufs[i][2].shape)

        def second(i):
            s1, r1, acc, s2, r2, s3, r3 = bufs[i]
            path = chunks[i][2]
            mb = xb if path == 0 else yb
            hop(i, 0).wait_recv()
            acc[...] = acc[...] + r1[...].astype(F32).reshape(acc.shape)
            for o in (0, 1):
                s2[o] = acc[block(path, 1 - mb, o)].astype(BF)
            hop(i, 1).start()

        def third(i):
            s1, r1, acc, s2, r2, s3, r3 = bufs[i]
            path = chunks[i][2]
            mb, ob = (xb, yb) if path == 0 else (yb, xb)
            hop(i, 1).wait_recv()
            s3[...] = (acc[block(path, mb, 1 - ob)] + r2[1 - ob].astype(F32)).astype(BF)
            hop(i, 2).start()

        def last(i):
            s1, r1, acc, s2, r2, s3, r3 = bufs[i]
            start, width, path = chunks[i]
            mb, ob = (xb, yb) if path == 0 else (yb, xb)
            kept = acc[block(path, mb, ob)] + r2[ob].astype(F32)
            hop(i, 2).wait_recv()
            w_out[:, start:start + width] = kept + r3[...].astype(F32)

        for i in range(0, nc, 2):
            for f in (send_first, own, second):
                f(i)
                f(i + 1)
        for f in (third, last):
            for i in range(nc):
                f(i)
        for i in range(nc):
            for stage in range(3):
                hop(i, stage).wait_send()

    for k in range(1, reach):
        @pl.when(d + k < n)
        def _(k=k):
            key_copy(k).wait_send()

        @pl.when(d - k >= 0)
        def _(k=k):
            part_copy(k, jnp.maximum(d - k, 0)).wait_send()
    for s in range(n - 1):
        for p in range(pieces):
            for direction in (1, -1):
                @pl.when(can_send(direction, s))
                def _(p=p, s=s, direction=direction):
                    relay(direction, s, p).wait_send()


def flush(gk, w, gk_out, w_out, sem):
    a = pltpu.make_async_copy(gk, gk_out, sem.at[0])
    b = pltpu.make_async_copy(w, w_out, sem.at[1])
    a.start()
    b.start()
    a.wait()
    b.wait()


def on_device(latent, queries, out_grad, hidden, doc_ids, clip_limits):
    n = lax.axis_size("ctx")
    groups = lax.axis_size("grp")
    tok, kw = latent.shape[1:]
    qd = queries.shape[1]
    seq = tok * n
    span = seq // 2 + qd
    reach = min(n, -(-span // tok))
    cols = hidden.shape[2]
    last = min(tok, -(-(span - (reach - 1) * tok) // 16) * 16)
    rows_of = [tok] * (reach - 1) + [last]
    ndocs = clip_limits.shape[1]
    scatter = groups == 8 and cols % 256 == 0 and cols >= 512 and kw % 64 == 0
    pieces = 2
    cfg = dict(n=n, tok=tok, kw=kw, qd=qd, reach=reach, rows_of=rows_of, span=span, ndocs=ndocs,
               pieces=pieces, scatter=scatter)
    rows = (HEADS // 2) * qd
    share = kw // 8
    dma = pltpu.SemaphoreType.DMA
    scratch = [
        pltpu.VMEM(queries.shape, BF),
        pltpu.VMEM(out_grad.shape, BF),
        pltpu.VMEM(hidden.shape, BF),
        pltpu.VMEM((rows, 2 * kw), BF),
        pltpu.VMEM((rows, 2 * LATENT), BF),
        pltpu.VMEM((reach - 1, tok, kw), BF),
        pltpu.VMEM((n, 1, tok), jnp.int32),
        pltpu.VMEM((reach - 1, tok, kw), BF),
        pltpu.VMEM((reach - 1, tok, kw), BF),
        pltpu.VMEM((n, tok, kw), BF),
        pltpu.VMEM((2, kw // 2, seq) if scatter else (kw, seq), BF),
        dma((3,)),
        dma((reach - 1,)), dma((reach - 1,)),
        dma((n - 1,)), dma((n - 1,)),
        dma((reach - 1,)), dma((reach - 1,)),
        dma((n - 1, pieces)), dma((n - 1, pieces)),
        dma((n - 1, pieces)), dma((n - 1, pieces)),
        pltpu.VMEM((1, tok, kw), BF),
    ]
    if scatter:
        chunks = col_chunks(cols)
        for _, w, _ in chunks:
            scratch += [
                pltpu.VMEM((kw // 2, w), BF), pltpu.VMEM((kw // 2, w), BF),
                pltpu.VMEM((4, share, w), F32),
                pltpu.VMEM((2, share, w), BF), pltpu.VMEM((2, share, w), BF),
                pltpu.VMEM((share, w), BF), pltpu.VMEM((share, w), BF),
            ]
        scratch += [dma((len(chunks), 3)), dma((len(chunks), 3))]
    vmem = pl.BlockSpec(memory_space=pltpu.VMEM)
    anywhere = pl.BlockSpec(memory_space=pl.ANY)
    grad_keys, weight = pl.pallas_call(
        functools.partial(body, cfg),
        out_shape=(
            pltpu.VMEM((1, kw, tok), BF),
            pltpu.VMEM((share if scatter else kw, cols), F32),
        ) if scatter else (
            jax.ShapeDtypeStruct((1, kw, tok), BF),
            jax.ShapeDtypeStruct((share if scatter else kw, cols), F32),
        ),
        in_specs=[vmem, vmem, vmem, anywhere, anywhere, anywhere],
        out_specs=(vmem, vmem),
        scratch_shapes=scratch,
        compiler_params=pltpu.CompilerParams(
            collective_id=0, has_side_effects=True, vmem_limit_bytes=60 * 1024 * 1024),
    )(jnp.swapaxes(latent, 1, 2), doc_ids, clip_limits, queries, out_grad, hidden)
    if not scatter:
        weight = lax.psum_scatter(weight, "grp", scatter_dimension=0, tiled=True)
    return (jnp.swapaxes(grad_keys, 1, 2), weight)


def solution(mesh):
    return jax.shard_map(
        on_device,
        mesh=mesh,
        in_specs=(
            P("grp", "ctx", None),
            P("grp", "ctx", None),
            P("grp", "ctx", None),
            P("grp", None, "ctx"),
            P("grp", "ctx"),
            P("grp", None),
        ),
        out_specs=(P("grp", "ctx", None), P("grp", "ctx")),
        check_vma=False,
    )
```

```python
import functools
import math

import jax
import jax.numpy as jnp
from jax import lax
from jax.experimental import pallas as pl
from jax.experimental.pallas import tpu as pltpu
from jax.sharding import PartitionSpec as P

LATENT = 512
HEADS = 128


score_scale = 192.0 ** (-0.5)
norm_eps = 1e-06

BF = jnp.bfloat16
F32 = jnp.float32


def dot(a, b, dims):
    return lax.dot_general(a, b, (dims, ((), ())), preferred_element_type=F32)


def body(cfg, *refs):
    n = cfg["n"]
    tok = cfg["tok"]
    kw = cfg["kw"]
    qd = cfg["qd"]
    reach = cfg["reach"]
    rows_of = cfg["rows_of"]
    span = cfg["span"]
    ndocs = cfg["ndocs"]
    pieces = cfg["pieces"]
    (lat_t, ids, lim, q_hbm, g_hbm, h_hbm, gk_out, w_out) = refs[:8]
    (qraw, graw, hid, qs, gs, kbuf, idbuf, psend, precv, full, scT, local_sem, key_s, key_r,
     id_s, id_r, part_s, part_r, up_s, up_r, dn_s, dn_r, lat) = refs[8:31]
    d = lax.axis_index("ctx")
    wide = -(-kw // 128) * 128
    pad = wide - kw
    pair = 2 * kw

    copy_q = pltpu.make_async_copy(q_hbm, qraw, local_sem.at[0])
    copy_g = pltpu.make_async_copy(g_hbm, graw, local_sem.at[1])
    copy_h = pltpu.make_async_copy(h_hbm, hid, local_sem.at[2])
    copy_q.start()
    copy_g.start()
    copy_h.start()

    def remote(src, dst, ss, rs, **where):
        axis, index = next(iter(where.items()))
        return pltpu.make_async_remote_copy(
            src_ref=src, dst_ref=dst, send_sem=ss, recv_sem=rs,
            device_id={axis: index}, device_id_type=pl.DeviceIdType.MESH,
        )

    barrier = pltpu.get_barrier_semaphore()
    for o in range(1, n):
        pl.semaphore_signal(barrier, inc=1, device_id={"ctx": lax.rem(d + o, n)},
                            device_id_type=pl.DeviceIdType.MESH)
    keys_t = jnp.concatenate([lat_t[0].astype(F32), jnp.zeros((pad, tok), F32)], axis=0)
    lat[0] = jnp.transpose(keys_t)[:, :kw].astype(BF)
    pl.semaphore_wait(barrier, n - 1)

    def key_copy(k):
        r = rows_of[k]
        return remote(lat.at[0, pl.ds(tok - r, r)], kbuf.at[k - 1, pl.ds(0, r)],
                      key_s.at[k - 1], key_r.at[k - 1], ctx=lax.rem(d + k, n))

    def id_copy(o):
        return remote(ids, idbuf.at[d], id_s.at[o - 1], id_r.at[o - 1], ctx=lax.rem(d + o, n))

    for k in range(1, reach):
        @pl.when(d + k < n)
        def _(k=k):
            key_copy(k).start()

    for o in range(1, n):
        id_copy(o).start()
    for k in range(1, reach):
        @pl.when(d - k < 0)
        def _(k=k):
            kbuf[k - 1] = jnp.zeros_like(kbuf[k - 1])
    idbuf[d] = ids[...]

    def repack(src, dst, width):
        group = 16 // qd

        def step(i, _):
            got = [
                src[0, :, pl.ds(pl.multiple_of((i * group + t) * width, 128), width)].astype(F32)
                for t in range(group)
            ]
            dst[pl.ds(pl.multiple_of(i * 16, 16), 16), :] = jnp.concatenate(got, axis=0).astype(BF)
            return 0

        lax.fori_loop(0, (HEADS // 2) // group, step, 0)

    copy_q.wait()
    repack(qraw, qs, pair)
    copy_g.wait()
    repack(graw, gs, 2 * LATENT)

    R = (HEADS // 2) * qd
    qrow = lax.broadcasted_iota(jnp.int32, (R, 1), 0) % qd
    own_ids = ids[...]
    qid = jnp.zeros((R, 1), jnp.int32)
    for i in range(qd):
        qid = jnp.where(qrow == i, own_ids[:, tok - qd + i:tok - qd + i + 1], qid)

    def query(par):
        return qs[:, 0:wide] if par == 0 else qs[:, pair - wide:pair]

    def grad(par):
        return gs[:, par * LATENT:(par + 1) * LATENT]

    def keys_of(k):
        return lat[0] if k == 0 else kbuf[k - 1, 0:rows_of[k], :]

    def block_products(k):
        kb = keys_of(k)
        zero = jnp.zeros((rows_of[k], pad), BF)
        padded = [jnp.concatenate([kb, zero], axis=1), jnp.concatenate([zero, kb], axis=1)]
        s = [dot(query(par), padded[par], ((1,), (1,))) for par in (0, 1)]
        dp = [dot(grad(par), kb[:, :LATENT], ((1,), (1,))) for par in (0, 1)]
        return s, dp

    products = [block_products(0)]

    for o in range(1, n):
        id_copy(o).wait_send()
        remote(ids, idbuf.at[lax.rem(d - o + n, n)], id_s.at[o - 1], id_r.at[o - 1],
               ctx=lax.rem(d + o, n)).wait_recv()
    for k in range(1, reach):
        @pl.when(d - k >= 0)
        def _(k=k):
            key_copy(k).wait_recv()
    for k in range(1, reach):
        products.append(block_products(k))

    allowed = []
    for k in range(reach):
        r = rows_of[k]
        row = own_ids if k == 0 else idbuf[jnp.maximum(d - k, 0)]
        row = row[:, tok - r:]
        lane = lax.broadcasted_iota(jnp.int32, (1, r), 1)
        ok = qid == row
        if k == 0:
            ok = ok & (lane <= tok - qd + qrow)
        else:
            reachable = jnp.where(lane + (tok - r) >= (k + 1) * tok - span, 1, 0)
            reachable = reachable * jnp.where(d - k >= 0, 1, 0)
            ok = ok & (reachable == 1)
        allowed.append(ok)

    dscores, probs = [[], []], [[], []]
    for par in (0, 1):
        s = [jnp.where(allowed[k], products[k][0][par] * score_scale, -1e30) for k in range(reach)]
        top = functools.reduce(jnp.maximum, [jnp.max(x, axis=1, keepdims=True) for x in s])
        w = [jnp.exp(x - top) for x in s]
        total = sum(jnp.sum(x, axis=1, keepdims=True) for x in w)
        w = [x / total for x in w]
        dps = [products[k][1][par] for k in range(reach)]
        rd = sum(jnp.sum(a * b, axis=1, keepdims=True) for a, b in zip(w, dps))
        for k in range(reach):
            dscores[par].append((w[k] * (dps[k] - rd) * score_scale).astype(BF))
            probs[par].append(w[k].astype(BF))

    def part_of(k):
        a = dot(dscores[0][k], query(0), ((0,), (0,)))[:, :kw]
        b = dot(dscores[1][k], query(1), ((0,), (0,)))[:, pad:pad + kw]
        v = dot(probs[0][k], grad(0), ((0,), (0,))) + dot(probs[1][k], grad(1), ((0,), (0,)))
        return (a + b + jnp.concatenate([v, jnp.zeros((rows_of[k], kw - LATENT), F32)], axis=1)).astype(BF)

    def part_copy(k, to):
        r = rows_of[k]
        return remote(psend.at[k - 1, pl.ds(0, r)], precv.at[k - 1, pl.ds(0, r)],
                      part_s.at[k - 1], part_r.at[k - 1], ctx=to)

    for k in range(1, reach):
        psend[k - 1, 0:rows_of[k], :] = part_of(k)

        @pl.when(d - k >= 0)
        def _(k=k):
            part_copy(k, jnp.maximum(d - k, 0)).start()

        @pl.when(d + k >= n)
        def _(k=k):
            precv[k - 1] = jnp.zeros_like(precv[k - 1])
    mine = part_of(0).astype(F32)

    eye = lax.broadcasted_iota(jnp.int32, (tok, tok), 0) == lax.broadcasted_iota(jnp.int32, (tok, tok), 1)
    doc_lane = lax.broadcasted_iota(jnp.int32, (1, 128), 1)
    member = []
    for j in range(n):
        col = jnp.sum(jnp.where(eye, idbuf[j], 0).astype(F32), axis=1, keepdims=True)
        member.append(jnp.where(col == doc_lane.astype(F32), 1.0, 0.0))

    for k in range(1, reach):
        @pl.when(d + k < n)
        def _(k=k):
            part_copy(k, jnp.maximum(d - k, 0)).wait_recv()
    for k in range(1, reach):
        r = rows_of[k]
        got = precv[k - 1, 0:r, :].astype(F32)
        if r < tok:
            got = jnp.concatenate([jnp.zeros((tok - r, kw), F32), got], axis=0)
        mine = mine + got
    mine_low = mine.astype(BF)
    full[d] = mine_low

    piece = tok // pieces

    def relay(direction, s, p):
        ss, rs = (up_s, up_r) if direction > 0 else (dn_s, dn_r)
        block = jnp.clip(d - direction * s, 0, n - 1)
        ref = full.at[block, pl.ds(p * piece, piece)]
        return remote(ref, ref, ss.at[s, p], rs.at[s, p], ctx=jnp.clip(d + direction, 0, n - 1))

    def arriving(direction, s, p):
        ss, rs = (up_s, up_r) if direction > 0 else (dn_s, dn_r)
        block = jnp.clip(d - direction * (s + 1), 0, n - 1)
        ref = full.at[block, pl.ds(p * piece, piece)]
        return remote(ref, ref, ss.at[s, p], rs.at[s, p], ctx=jnp.clip(d + direction, 0, n - 1))

    def can_send(direction, s):
        if direction > 0:
            return (d - s >= 0) & (d + 1 < n)
        return (d + s < n) & (d - 1 >= 0)

    def will_get(direction, s):
        return d - s - 1 >= 0 if direction > 0 else d + s + 1 < n

    for p in range(pieces):
        for direction in (1, -1):
            @pl.when(can_send(direction, 0))
            def _(p=p, direction=direction):
                relay(direction, 0, p).start()
    padded_out = jnp.concatenate([mine_low.astype(F32), jnp.zeros((tok, pad), F32)], axis=1)
    gk_out[0] = jnp.transpose(padded_out)[:kw].astype(BF)
    for s in range(n - 1):
        for p in range(pieces):
            for direction in (1, -1):
                @pl.when(will_get(direction, s))
                def _(p=p, s=s, direction=direction):
                    arriving(direction, s, p).wait_recv()
                if s + 1 < n - 1:
                    @pl.when(can_send(direction, s + 1))
                    def _(p=p, s=s, direction=direction):
                        relay(direction, s + 1, p).start()

    norms = jnp.zeros((1, 128), F32)
    for j in range(n):
        v = full[j].astype(F32)
        norms = norms + jnp.sum(member[j] * jnp.sum(v * v, axis=1, keepdims=True), axis=0, keepdims=True)
    limits = lim[...]
    if ndocs < 128:
        limits = jnp.concatenate([limits, jnp.zeros((1, 128 - ndocs), F32)], axis=1)
    factor = jnp.minimum(1.0, limits / jnp.sqrt(norms + norm_eps))
    for j in range(n):
        f = jnp.sum(member[j] * factor, axis=1, keepdims=True)
        scaled = (full[j].astype(F32) * f).astype(BF).astype(F32)
        scaled = jnp.concatenate([scaled, jnp.zeros((tok, pad), F32)], axis=1)
        turned = jnp.transpose(scaled)
        scT[:, j * tok:(j + 1) * tok] = turned[:kw].astype(BF)

    copy_h.wait()
    w_out[...] = dot(scT[...], hid[0], ((1,), (0,)))

    for k in range(1, reach):
        @pl.when(d + k < n)
        def _(k=k):
            key_copy(k).wait_send()

        @pl.when(d - k >= 0)
        def _(k=k):
            part_copy(k, jnp.maximum(d - k, 0)).wait_send()
    for s in range(n - 1):
        for p in range(pieces):
            for direction in (1, -1):
                @pl.when(can_send(direction, s))
                def _(p=p, s=s, direction=direction):
                    relay(direction, s, p).wait_send()


def flush(gk, w, gk_out, w_out, sem):
    a = pltpu.make_async_copy(gk, gk_out, sem.at[0])
    b = pltpu.make_async_copy(w, w_out, sem.at[1])
    a.start()
    b.start()
    a.wait()
    b.wait()


def pair_body(cfg, *refs):
    n = cfg["n"]
    tok = cfg["tok"]
    kw = cfg["kw"]
    qd = cfg["qd"]
    halo = cfg["halo"]
    ndocs = cfg["ndocs"]
    splits = cfg["splits"]
    seq = n * tok
    wide = -(-kw // 128) * 128
    pad = wide - kw
    share = kw // 8
    np_ = len(splits)
    offs = [sum(splits[:p]) for p in range(np_)]
    (lat_hbm, ids_hbm, lim_hbm, q_hbm, g_hbm, h_hbm, gk_out, w_out,
     lat_t, lat, ids, lim, qraw, graw, hid, qs, gs, kbuf, krot, kgot, lath, hkey, idbuf,
     psend, precv, hsend, hrecv, ownb, own2, full, gkr, nbuf, lhs,
     loc, id_s, id_r, key_s, key_r, hid_s, hid_r, part_s, part_r, halo_s, halo_r,
     own_s, own_r, gk_s, gk_r, nrm_s, nrm_r, blk_s, blk_r, rs_s, rs_r) = refs[:54]
    tail = refs[54:]
    d = lax.axis_index("ctx")
    m = lax.axis_index("grp")
    c = lax.rem(m, 2)
    xb = lax.rem(m // 2, 2)
    yb = lax.rem(m // 4, 2)
    base = m - c
    mate = base + 1 - c
    flip_x = m + 2 - 4 * xb
    flip_y = m + 4 - 8 * yb
    cols = w_out.shape[1]
    wing = cols // 2

    def remote(src, dst, ss, rs, **where):
        return pltpu.make_async_remote_copy(
            src_ref=src, dst_ref=dst, send_sem=ss, recv_sem=rs,
            device_id=where, device_id_type=pl.DeviceIdType.MESH,
        )

    loads = [
        pltpu.make_async_copy(lat_hbm, lat_t, loc.at[0]),
        pltpu.make_async_copy(ids_hbm, ids, loc.at[1]),
        pltpu.make_async_copy(q_hbm, qraw, loc.at[2]),
        pltpu.make_async_copy(g_hbm, graw, loc.at[3]),
        pltpu.make_async_copy(lim_hbm, lim, loc.at[4]),
        pltpu.make_async_copy(h_hbm.at[0], hid.at[c], loc.at[5]),
    ]
    for copy in loads:
        copy.start()

    barrier = pltpu.get_barrier_semaphore()

    def greet(**where):
        pl.semaphore_signal(barrier, inc=1, device_id=where, device_id_type=pl.DeviceIdType.MESH)

    for o in range(n):
        if o:
            greet(ctx=lax.rem(d + o, n), grp=m)
        greet(ctx=lax.rem(d + o, n), grp=mate)
    greet(grp=flip_x)
    greet(grp=flip_y)

    loads[0].wait()
    keys_t = jnp.concatenate([lat_t[0].astype(F32), jnp.zeros((pad, tok), F32)], axis=0)
    keys = jnp.transpose(keys_t)
    lat[...] = keys.astype(BF)
    near = tok // 2
    rope = kw - LATENT
    krot[...] = jnp.concatenate([keys[:near, LATENT:kw], keys[near:, LATENT:kw]], axis=1).astype(BF)
    lath[...] = keys[tok - halo:].astype(BF)
    loads[1].wait()
    pl.semaphore_wait(barrier, 2 * n + 1)

    def id_copy(k):
        return remote(ids, idbuf.at[k - 1], id_s.at[k - 1], id_r.at[k - 1], ctx=lax.rem(d + k, n))

    def key_copy(k):
        if k == 1:
            return [
                remote(lat.at[:, pl.ds(0, LATENT)], kbuf.at[pl.ds(0, tok), pl.ds(0, LATENT)],
                       key_s.at[0], key_r.at[0], ctx=lax.rem(d + 1, n)),
                remote(krot, kgot, key_s.at[2], key_r.at[2], ctx=lax.rem(d + 1, n)),
            ]
        return [remote(lath, hkey, key_s.at[1], key_r.at[1], ctx=lax.rem(d + 2, n))]

    for k in (2, 1):
        @pl.when(d + k < n)
        def _(k=k):
            id_copy(k).start()
            for copy in key_copy(k):
                copy.start()

    hid_copy = remote(h_hbm.at[0], hid.at[c], hid_s.at[0], hid_r.at[0], grp=mate)
    hid_copy.start()

    @pl.when(d < 1)
    def _():
        kbuf[0:tok, :] = jnp.zeros((tok, wide), BF)
        kgot[...] = jnp.zeros_like(kgot)
        idbuf[0] = jnp.zeros_like(idbuf[0])

    @pl.when(d < 2)
    def _():
        hkey[...] = jnp.zeros_like(hkey)
        idbuf[1] = jnp.zeros_like(idbuf[1])

    group = 16 // qd
    R = (HEADS // 2) * qd

    def repack(src, dst, width):
        def step(i, _):
            got = [
                src[0, :, pl.ds(pl.multiple_of((i * group + t) * 2 * width, 128), 2 * width)].astype(F32)
                for t in range(group)
            ]
            got = jnp.concatenate(got, axis=0)
            for par in (0, 1):
                one = got[:, par * width:(par + 1) * width]
                if width % 128:
                    one = jnp.concatenate([one, jnp.zeros((16, pad), F32)], axis=1)
                dst[pl.ds(pl.multiple_of(par * R + i * 16, 16), 16), :] = one.astype(BF)
            return 0

        lax.fori_loop(0, (HEADS // 2) // group, step, 0)

    loads[2].wait()
    repack(qraw, qs, kw)
    loads[3].wait()
    repack(graw, gs, LATENT)

    def turn_ids(row):
        return jnp.transpose(jnp.broadcast_to(row.astype(F32), (tok, tok)))

    def across(x):
        return jnp.concatenate([x] * (2 * R // tok), axis=1)

    qrow = lax.broadcasted_iota(jnp.int32, (1, tok), 1) % qd
    own_ids = ids[...]
    qid = jnp.zeros((1, tok), F32)
    for i in range(qd):
        qid = jnp.where(qrow == i, own_ids[:, tok - qd + i:tok - qd + i + 1].astype(F32), qid)

    def block_products(keys):
        return (dot(keys, qs[...], ((1,), (1,))), dot(keys[:, :LATENT], gs[...], ((1,), (1,))))

    key_row = lax.broadcasted_iota(jnp.int32, (tok, tok), 0)
    s0, dp0 = block_products(lat[...])
    ok0 = jnp.where(turn_ids(own_ids) == qid, 1, 0) * jnp.where(key_row <= tok - qd + qrow, 1, 0)
    s0 = jnp.where(across(ok0) == 1, s0 * score_scale, -1e30)
    top0 = jnp.max(s0, axis=0, keepdims=True)

    for k in (2, 1):
        @pl.when(d >= k)
        def _(k=k):
            id_copy(k).wait_recv()
            for copy in key_copy(k):
                copy.wait_recv()
    got = kgot[...].astype(F32)
    got = jnp.concatenate([got[:, :rope], got[:, rope:]], axis=0)
    kbuf[0:tok, LATENT:wide] = jnp.concatenate([got, jnp.zeros((tok, wide - kw), F32)], axis=1).astype(BF)
    kbuf[tok:tok + 16, :] = jnp.concatenate([jnp.zeros((16 - halo, wide), F32), hkey[...].astype(F32)], axis=0).astype(BF)
    s1, dp1 = block_products(kbuf[...])
    ok1 = jnp.where(turn_ids(idbuf[0]) == qid, 1, 0)
    ok1 = ok1 * jnp.where(key_row >= 2 * tok - cfg["span"], 1, 0) * jnp.where(d >= 1, 1, 0)
    ok2 = jnp.where(turn_ids(idbuf[1]) == qid, 1, 0)
    ok2 = ok2 * jnp.where(key_row >= 3 * tok - cfg["span"], 1, 0) * jnp.where(d >= 2, 1, 0)
    ok1 = jnp.concatenate([ok1, ok2[tok - 16:]], axis=0)
    s1 = jnp.where(across(ok1) == 1, s1 * score_scale, -1e30)
    top = jnp.maximum(top0, jnp.max(s1, axis=0, keepdims=True))
    w0, w1 = jnp.exp(s0 - top), jnp.exp(s1 - top)
    scale = 1.0 / (jnp.sum(w0, axis=0, keepdims=True) + jnp.sum(w1, axis=0, keepdims=True))
    w0, w1 = w0 * scale, w1 * scale
    rd = jnp.sum(w0 * dp0, axis=0, keepdims=True) + jnp.sum(w1 * dp1, axis=0, keepdims=True)

    def part_of(w, dp):
        a = dot((w * (dp - rd) * score_scale).astype(BF), qs[...], ((1,), (0,)))
        v = dot(w.astype(BF), gs[...], ((1,), (0,)))
        return a + jnp.concatenate([v, jnp.zeros((v.shape[0], wide - LATENT), F32)], axis=1)

    def halves(turned):
        out = []
        for h in (0, 1):
            rows = []
            for p in range(np_):
                for q in range(4):
                    start = share * (2 * q + h) + offs[p]
                    rows.append(turned[start:start + splits[p]])
            out.append(jnp.concatenate(rows, axis=0))
        return out

    def halo_copy(h):
        return remote(hsend, hrecv.at[c], halo_s.at[h], halo_r.at[c],
                      ctx=jnp.maximum(d - 2, 0), grp=base + h)

    def part_copy(h, p):
        rows = pl.ds(4 * offs[p], 4 * splits[p])
        return remote(psend.at[h, rows], precv.at[c, rows], part_s.at[h, p], part_r.at[c, p],
                      ctx=jnp.maximum(d - 1, 0), grp=base + h)

    part1 = part_of(w1, dp1)
    hsend[...] = part1[tok + 16 - halo:].astype(BF)

    @pl.when(d >= 2)
    def _():
        for h in (0, 1):
            halo_copy(h).start()

    turned = halves(jnp.transpose(part1[:tok]))
    for h in (0, 1):
        psend[h] = turned[h].astype(BF)

    @pl.when(d >= 1)
    def _():
        for p in range(np_):
            for h in (0, 1):
                part_copy(h, p).start()

    @pl.when(d + 1 >= n)
    def _():
        precv[...] = jnp.zeros_like(precv)

    @pl.when(d + 2 >= n)
    def _():
        hrecv[...] = jnp.zeros_like(hrecv)

    turned = halves(jnp.transpose(part_of(w0, dp0)))
    for h in (0, 1):
        ownb[h] = turned[h].astype(BF)
    own_copy = remote(ownb.at[1 - c], own2.at[c], own_s.at[0], own_r.at[0], grp=mate)
    own_copy.start()
    own2[c] = ownb[c]
    own_copy.wait_recv()

    def rows_at(p):
        return pl.ds(8 * offs[p], 8 * splits[p])

    steps = (-1, 1, -2, 2)

    def spread(o, p):
        i = steps.index(o)
        ref = full.at[d, rows_at(p)]
        return remote(ref, ref, blk_s.at[i, p], blk_r.at[i, p], ctx=jnp.clip(d + o, 0, n - 1))

    def spread_from(o, p):
        i = steps.index(o)
        ref = full.at[jnp.clip(d - o, 0, n - 1), rows_at(p)]
        return remote(ref, ref, blk_s.at[i, p], blk_r.at[i, p], ctx=jnp.clip(d - o, 0, n - 1))

    def pass_end(o, p):
        i = 4 if o < 0 else 5
        ref = full.at[n - 1 if o < 0 else 0, rows_at(p)]
        return remote(ref, ref, blk_s.at[i, p], blk_r.at[i, p], ctx=jnp.clip(d + o, 0, n - 1))

    def reaches(o):
        return (d + o >= 0) & (d + o < n)

    def comes(o):
        return (d - o >= 0) & (d - o < n)

    def passes(o):
        return d == (1 if o < 0 else n - 2)

    def ends(o):
        return d == (0 if o < 0 else n - 1)

    def halo_from(g):
        return remote(hsend, hrecv.at[g], halo_s.at[0], halo_r.at[g], grp=mate)

    def part_from(g, p):
        rows = pl.ds(4 * offs[p], 4 * splits[p])
        return remote(psend.at[0, rows], precv.at[g, rows], part_s.at[0, p], part_r.at[g, p], grp=mate)

    @pl.when(d + 2 < n)
    def _():
        for g in (0, 1):
            halo_from(g).wait_recv()

    side = []
    for g in (0, 1):
        block = jnp.concatenate([jnp.zeros((tok - halo, wide), F32), hrecv[g].astype(F32)], axis=0)
        turned = halves(jnp.transpose(block))
        side.append(jnp.where(c == 0, turned[0], turned[1]))

    def spread_all(p):
        for o in steps:
            @pl.when(reaches(o))
            def _(o=o):
                spread(o, p).start()

    token_norm = [jnp.zeros((1, tok), F32) for _ in (0, 1)]
    for p in range(np_):
        @pl.when(d + 1 < n)
        def _(p=p):
            for g in (0, 1):
                part_from(g, p).wait_recv()
        lo, size = 4 * offs[p], 4 * splits[p]
        for g in (0, 1):
            value = own2[g, lo:lo + size].astype(F32) + precv[g, lo:lo + size].astype(F32)
            value = (value + side[g][lo:lo + size]).astype(BF)
            full[d, 2 * lo + g * size:2 * lo + (g + 1) * size] = value
            value = value.astype(F32)
            token_norm[g] = token_norm[g] + jnp.sum(value * value, axis=0, keepdims=True)
        if p == 0:
            spread_all(p)

    loads[4].wait()
    limits = jnp.concatenate([lim[...], jnp.zeros((1, tok - ndocs), F32)], axis=1)
    nbuf[c, d] = jnp.concatenate(
        token_norm + [own_ids.astype(F32), limits, jnp.zeros((4, tok), F32)], axis=0)

    def norm_copy(o, flip):
        i = 2 * o + flip - 1
        ref = nbuf.at[c, d]
        return remote(ref, ref, nrm_s.at[i], nrm_r.at[i], ctx=lax.rem(d + o, n), grp=mate if flip else m)

    def norm_from(o, flip):
        i = 2 * o + flip - 1
        ref = nbuf.at[1 - c if flip else c, lax.rem(d - o + n, n)]
        return remote(ref, ref, nrm_s.at[i], nrm_r.at[i], ctx=lax.rem(d + o, n), grp=mate if flip else m)

    peers = [(o, flip) for o in range(n) for flip in (0, 1) if o or flip]
    for o, flip in peers:
        norm_copy(o, flip).start()
    for p in range(1, np_):
        spread_all(p)

    def gk_copy(p):
        lo, size = 4 * offs[p], 4 * splits[p]
        src = full.at[d, pl.ds(pl.multiple_of(2 * lo + (1 - c) * size, 16), size)]
        return remote(src, gkr.at[pl.ds(lo, size)], gk_s.at[p], gk_r.at[p], grp=mate)

    for p in range(np_):
        gk_copy(p).start()

    factors = []

    def make_factors():
        for o, flip in peers:
            norm_from(o, flip).wait_recv()
        rows = -(-ndocs // 8) * 8
        sub = lax.broadcasted_iota(jnp.int32, (rows, tok), 0).astype(F32)
        lane = lax.broadcasted_iota(jnp.int32, (rows, tok), 1).astype(F32)
        for g in (0, 1):
            member = [jnp.where(nbuf[g, b, 2:3] == sub, 1.0, 0.0) for b in range(n)]
            norms = sum(
                jnp.sum(member[b] * (nbuf[0, b, g:g + 1] + nbuf[1, b, g:g + 1]), axis=1, keepdims=True)
                for b in range(n))
            top = jnp.sum(jnp.where(lane == sub, nbuf[g, 0, 3:4], 0.0), axis=1, keepdims=True)
            factor = jnp.minimum(1.0, top / jnp.sqrt(norms + norm_eps))
            factors.append([jnp.sum(member[b] * factor, axis=0, keepdims=True) for b in range(n)])

    def forward(p):
        for o in (-1, 1):
            @pl.when(passes(o))
            def _(o=o):
                spread_from(2 * o, p).wait_recv()
                pass_end(o, p).start()

    def gather(p):
        for o in steps:
            keep = comes(o)
            if o in (-2, 2):
                keep = keep & jnp.logical_not(passes(o // 2))

            @pl.when(keep)
            def _(o=o):
                spread_from(o, p).wait_recv()
        for o in (-1, 1):
            @pl.when(ends(o))
            def _(o=o):
                pass_end(o, p).wait_recv()

    bufs = [[tail[5 * (2 * p + w):5 * (2 * p + w) + 5] for w in (0, 1)] for p in range(np_)]

    def hop(p, w, stage):
        first, back, second, back2, _ = bufs[p][w]
        where = (flip_x, flip_y) if w == 0 else (flip_y, flip_x)
        src, dst = (first, back) if stage == 0 else (second, back2)
        return remote(src, dst, rs_s.at[p, w, stage], rs_r.at[p, w, stage], grp=where[stage])

    def chip(w, moving, other):
        return other * 2 + moving if w == 0 else moving * 2 + other

    def product(p):
        lo, size = 4 * offs[p], 4 * splits[p]
        for g in (0, 1):
            for b in range(n):
                value = full[b, 2 * lo + g * size:2 * lo + (g + 1) * size].astype(F32)
                at = (g * n + b) * tok
                lhs[lo:lo + size, at:at + tok] = (value * factors[g][b]).astype(BF)
        for w in (0, 1):
            first, _, _, _, total = bufs[p][w]
            out = sum(
                dot(lhs[lo:lo + size, g * seq:(g + 1) * seq], hid[g, :, w * wing:(w + 1) * wing], ((1,), (0,)))
                for g in (0, 1))
            total[...] = out.reshape(total.shape)
            mb = xb if w == 0 else yb
            for o in (0, 1):
                first[o] = total[chip(w, 1 - mb, o)].astype(BF)
            hop(p, w, 0).start()

    def pass_on(p):
        for w in (0, 1):
            _, back, second, _, total = bufs[p][w]
            mb, ob = (xb, yb) if w == 0 else (yb, xb)
            hop(p, w, 0).wait_recv()
            second[...] = (total[chip(w, mb, 1 - ob)] + back[1 - ob].astype(F32)).astype(BF)
            hop(p, w, 1).start()

    def last(p):
        for w in (0, 1):
            _, back, _, back2, total = bufs[p][w]
            mb, ob = (xb, yb) if w == 0 else (yb, xb)
            kept = total[chip(w, mb, ob)] + back[ob].astype(F32)
            hop(p, w, 1).wait_recv()
            w_out[offs[p]:offs[p] + splits[p], w * wing:(w + 1) * wing] = kept + back2[...].astype(F32)

    def write_keys():
        for p in range(np_):
            gk_copy(p).wait_recv()
        order = [None] * (8 * np_)
        for p in range(np_):
            lo, size = 4 * offs[p], splits[p]
            near = [full[d, 2 * lo + g * 4 * size:2 * lo + (g + 1) * 4 * size].astype(F32) for g in (0, 1)]
            near = jnp.where(c == 0, near[0], near[1])
            far = gkr[lo:lo + 4 * size].astype(F32)
            for h in (0, 1):
                value = jnp.where(c == h, near, far)
                for q in range(4):
                    order[(2 * q + h) * np_ + p] = value[q * size:(q + 1) * size]
        gk_out[0] = jnp.concatenate(order, axis=0).astype(BF)

    forward(0)
    make_factors()
    loads[5].wait()
    hid_copy.wait_recv()
    for p in range(np_):
        if p + 1 < np_:
            forward(p + 1)
        gather(p)
        product(p)
        if p == 0:
            write_keys()
        if p >= 1:
            pass_on(p - 1)
        if p >= 2:
            last(p - 2)
    pass_on(np_ - 1)
    if np_ >= 2:
        last(np_ - 2)
    last(np_ - 1)

    for k in (1, 2):
        @pl.when(d + k < n)
        def _(k=k):
            id_copy(k).wait_send()
            for copy in key_copy(k):
                copy.wait_send()
    hid_copy.wait_send()

    @pl.when(d >= 2)
    def _():
        for h in (0, 1):
            halo_copy(h).wait_send()

    @pl.when(d >= 1)
    def _():
        for p in range(np_):
            for h in (0, 1):
                part_copy(h, p).wait_send()
    own_copy.wait_send()
    for p in range(np_):
        gk_copy(p).wait_send()
    for o, flip in peers:
        norm_copy(o, flip).wait_send()
    for p in range(np_):
        for o in steps:
            @pl.when(reaches(o))
            def _(p=p, o=o):
                spread(o, p).wait_send()
        for o in (-1, 1):
            @pl.when(passes(o))
            def _(p=p, o=o):
                pass_end(o, p).wait_send()
    for p in range(np_):
        for w in (0, 1):
            for stage in (0, 1):
                hop(p, w, stage).wait_send()


def pair_scratch(cfg, latent, queries, out_grad, hidden, clip_limits):
    n, tok, kw, halo = cfg["n"], cfg["tok"], cfg["kw"], cfg["halo"]
    splits = cfg["splits"]
    np_ = len(splits)
    half = kw // 2
    wide = -(-kw // 128) * 128
    rows = (HEADS // 2) * cfg["qd"]
    cols = hidden.shape[2]
    seq = n * tok
    dma = pltpu.SemaphoreType.DMA
    v = pltpu.VMEM
    scratch = [
        v((1, kw, tok), BF), v((tok, wide), BF), v((1, tok), jnp.int32), v(clip_limits.shape, F32),
        v(queries.shape, BF), v(out_grad.shape, BF), v((2, seq, cols), BF),
        v((2 * rows, wide), BF), v((2 * rows, LATENT), BF),
        v((tok + 16, wide), BF), v((tok // 2, 2 * (kw - LATENT)), BF), v((tok // 2, 2 * (kw - LATENT)), BF),
        v((halo, wide), BF), v((halo, wide), BF), v((2, 1, tok), jnp.int32),
        v((2, half, tok), BF), v((2, half, tok), BF), v((halo, wide), BF), v((2, halo, wide), BF),
        v((2, half, tok), BF), v((2, half, tok), BF), v((n, kw, tok), BF), v((half, tok), BF),
        v((2, n, 8, tok), F32), v((half, 2 * seq), BF),
        dma((6,)), dma((2,)), dma((2,)), dma((3,)), dma((3,)), dma((1,)), dma((1,)),
        dma((2, np_)), dma((2, np_)), dma((2,)), dma((2,)),
        dma((1,)), dma((1,)), dma((np_,)), dma((np_,)),
        dma((2 * n,)), dma((2 * n,)),
        dma((6, np_)), dma((6, np_)),
        dma((np_, 2, 2)), dma((np_, 2, 2)),
    ]
    for size in splits:
        for _ in (0, 1):
            scratch += [
                v((2, size, cols // 2), BF), v((2, size, cols // 2), BF),
                v((size, cols // 2), BF), v((size, cols // 2), BF),
                v((4, size, cols // 2), F32),
            ]
    return scratch


def row_splits(share):
    units = share // 8
    cuts = [0] + [units * p // 9 for p in (3, 6)] + [units]
    return tuple(8 * (b - a) for a, b in zip(cuts, cuts[1:]) if b > a)


def pair_call(cfg, latent, queries, out_grad, hidden, doc_ids, clip_limits):
    anywhere = pl.BlockSpec(memory_space=pl.ANY)
    vmem = pl.BlockSpec(memory_space=pltpu.VMEM)
    tok, kw = cfg["tok"], cfg["kw"]
    grad_keys, weight = pl.pallas_call(
        functools.partial(pair_body, cfg),
        out_shape=(
            pltpu.VMEM((1, kw, tok), BF),
            pltpu.VMEM((kw // 8, hidden.shape[2]), F32),
        ),
        in_specs=[anywhere] * 6,
        out_specs=(vmem, vmem),
        scratch_shapes=pair_scratch(cfg, latent, queries, out_grad, hidden, clip_limits),
        compiler_params=pltpu.CompilerParams(
            collective_id=0, has_side_effects=True, vmem_limit_bytes=56 * 1024 * 1024),
    )(jnp.swapaxes(latent, 1, 2), doc_ids, clip_limits, queries, out_grad, hidden)
    return (jnp.swapaxes(grad_keys, 1, 2), weight)


def on_device(latent, queries, out_grad, hidden, doc_ids, clip_limits):
    n = lax.axis_size("ctx")
    groups = lax.axis_size("grp")
    tok, kw = latent.shape[1:]
    qd = queries.shape[1]
    seq = tok * n
    span = seq // 2 + qd
    reach = min(n, -(-span // tok))
    cols = hidden.shape[2]
    last = min(tok, -(-(span - (reach - 1) * tok) // 16) * 16)
    rows_of = [tok] * (reach - 1) + [last]
    ndocs = clip_limits.shape[1]
    share = kw // 8
    paired = (groups == 8 and n == 4 and reach == 3 and last <= tok and cols % 256 == 0 and kw % 64 == 0
              and tok % 128 == 0 and ndocs <= tok and span <= 2 * tok + 16 and 2 * (kw - LATENT) == 128)
    if paired:
        cfg = dict(n=n, tok=tok, kw=kw, qd=qd, halo=-(-(span - 2 * tok) // 4) * 4, span=span, ndocs=ndocs, splits=row_splits(share))
        return pair_call(cfg, latent, queries, out_grad, hidden, doc_ids, clip_limits)
    pieces = 2
    cfg = dict(n=n, tok=tok, kw=kw, qd=qd, reach=reach, rows_of=rows_of, span=span, ndocs=ndocs,
               pieces=pieces)
    rows = (HEADS // 2) * qd
    dma = pltpu.SemaphoreType.DMA
    scratch = [
        pltpu.VMEM(queries.shape, BF),
        pltpu.VMEM(out_grad.shape, BF),
        pltpu.VMEM(hidden.shape, BF),
        pltpu.VMEM((rows, 2 * kw), BF),
        pltpu.VMEM((rows, 2 * LATENT), BF),
        pltpu.VMEM((reach - 1, tok, kw), BF),
        pltpu.VMEM((n, 1, tok), jnp.int32),
        pltpu.VMEM((reach - 1, tok, kw), BF),
        pltpu.VMEM((reach - 1, tok, kw), BF),
        pltpu.VMEM((n, tok, kw), BF),
        pltpu.VMEM((kw, seq), BF),
        dma((3,)),
        dma((reach - 1,)), dma((reach - 1,)),
        dma((n - 1,)), dma((n - 1,)),
        dma((reach - 1,)), dma((reach - 1,)),
        dma((n - 1, pieces)), dma((n - 1, pieces)),
        dma((n - 1, pieces)), dma((n - 1, pieces)),
        pltpu.VMEM((1, tok, kw), BF),
    ]
    vmem = pl.BlockSpec(memory_space=pltpu.VMEM)
    anywhere = pl.BlockSpec(memory_space=pl.ANY)
    grad_keys, weight = pl.pallas_call(
        functools.partial(body, cfg),
        out_shape=(
            jax.ShapeDtypeStruct((1, kw, tok), BF),
            jax.ShapeDtypeStruct((kw, cols), F32),
        ),
        in_specs=[vmem, vmem, vmem, anywhere, anywhere, anywhere],
        out_specs=(vmem, vmem),
        scratch_shapes=scratch,
        compiler_params=pltpu.CompilerParams(
            collective_id=0, has_side_effects=True, vmem_limit_bytes=60 * 1024 * 1024),
    )(jnp.swapaxes(latent, 1, 2), doc_ids, clip_limits, queries, out_grad, hidden)
    weight = lax.psum_scatter(weight, "grp", scatter_dimension=0, tiled=True)
    return (jnp.swapaxes(grad_keys, 1, 2), weight)


def solution(mesh):
    return jax.shard_map(
        on_device,
        mesh=mesh,
        in_specs=(
            P("grp", "ctx", None),
            P("grp", "ctx", None),
            P("grp", "ctx", None),
            P("grp", None, "ctx"),
            P("grp", "ctx"),
            P("grp", None),
        ),
        out_specs=(P("grp", "ctx", None), P("grp", "ctx")),
        check_vma=False,
    )
```

```python
import functools
import math

import jax
import jax.numpy as jnp
from jax import lax
from jax.experimental import pallas as pl
from jax.experimental.pallas import tpu as pltpu
from jax.sharding import PartitionSpec as P

LATENT = 512
HEADS = 128


score_scale = 192.0 ** (-0.5)
norm_eps = 1e-06

BF = jnp.bfloat16
F32 = jnp.float32


def dot(a, b, dims):
    return lax.dot_general(a, b, (dims, ((), ())), preferred_element_type=F32)


def body(cfg, *refs):
    n = cfg["n"]
    tok = cfg["tok"]
    kw = cfg["kw"]
    qd = cfg["qd"]
    reach = cfg["reach"]
    rows_of = cfg["rows_of"]
    span = cfg["span"]
    ndocs = cfg["ndocs"]
    pieces = cfg["pieces"]
    (lat_t, ids, lim, q_hbm, g_hbm, h_hbm, gk_out, w_out) = refs[:8]
    (qraw, graw, hid, qs, gs, kbuf, idbuf, psend, precv, full, scT, local_sem, key_s, key_r,
     id_s, id_r, part_s, part_r, up_s, up_r, dn_s, dn_r, lat) = refs[8:31]
    d = lax.axis_index("ctx")
    wide = -(-kw // 128) * 128
    pad = wide - kw
    pair = 2 * kw

    copy_q = pltpu.make_async_copy(q_hbm, qraw, local_sem.at[0])
    copy_g = pltpu.make_async_copy(g_hbm, graw, local_sem.at[1])
    copy_h = pltpu.make_async_copy(h_hbm, hid, local_sem.at[2])
    copy_q.start()
    copy_g.start()
    copy_h.start()

    def remote(src, dst, ss, rs, **where):
        axis, index = next(iter(where.items()))
        return pltpu.make_async_remote_copy(
            src_ref=src, dst_ref=dst, send_sem=ss, recv_sem=rs,
            device_id={axis: index}, device_id_type=pl.DeviceIdType.MESH,
        )

    barrier = pltpu.get_barrier_semaphore()
    for o in range(1, n):
        pl.semaphore_signal(barrier, inc=1, device_id={"ctx": lax.rem(d + o, n)},
                            device_id_type=pl.DeviceIdType.MESH)
    keys_t = jnp.concatenate([lat_t[0].astype(F32), jnp.zeros((pad, tok), F32)], axis=0)
    lat[0] = jnp.transpose(keys_t)[:, :kw].astype(BF)
    pl.semaphore_wait(barrier, n - 1)

    def key_copy(k):
        r = rows_of[k]
        return remote(lat.at[0, pl.ds(tok - r, r)], kbuf.at[k - 1, pl.ds(0, r)],
                      key_s.at[k - 1], key_r.at[k - 1], ctx=lax.rem(d + k, n))

    def id_copy(o):
        return remote(ids, idbuf.at[d], id_s.at[o - 1], id_r.at[o - 1], ctx=lax.rem(d + o, n))

    for k in range(1, reach):
        @pl.when(d + k < n)
        def _(k=k):
            key_copy(k).start()

    for o in range(1, n):
        id_copy(o).start()
    for k in range(1, reach):
        @pl.when(d - k < 0)
        def _(k=k):
            kbuf[k - 1] = jnp.zeros_like(kbuf[k - 1])
    idbuf[d] = ids[...]

    def repack(src, dst, width):
        group = 16 // qd

        def step(i, _):
            got = [
                src[0, :, pl.ds(pl.multiple_of((i * group + t) * width, 128), width)].astype(F32)
                for t in range(group)
            ]
            dst[pl.ds(pl.multiple_of(i * 16, 16), 16), :] = jnp.concatenate(got, axis=0).astype(BF)
            return 0

        lax.fori_loop(0, (HEADS // 2) // group, step, 0)

    copy_q.wait()
    repack(qraw, qs, pair)
    copy_g.wait()
    repack(graw, gs, 2 * LATENT)

    R = (HEADS // 2) * qd
    qrow = lax.broadcasted_iota(jnp.int32, (R, 1), 0) % qd
    own_ids = ids[...]
    qid = jnp.zeros((R, 1), jnp.int32)
    for i in range(qd):
        qid = jnp.where(qrow == i, own_ids[:, tok - qd + i:tok - qd + i + 1], qid)

    def query(par):
        return qs[:, 0:wide] if par == 0 else qs[:, pair - wide:pair]

    def grad(par):
        return gs[:, par * LATENT:(par + 1) * LATENT]

    def keys_of(k):
        return lat[0] if k == 0 else kbuf[k - 1, 0:rows_of[k], :]

    def block_products(k):
        kb = keys_of(k)
        zero = jnp.zeros((rows_of[k], pad), BF)
        padded = [jnp.concatenate([kb, zero], axis=1), jnp.concatenate([zero, kb], axis=1)]
        s = [dot(query(par), padded[par], ((1,), (1,))) for par in (0, 1)]
        dp = [dot(grad(par), kb[:, :LATENT], ((1,), (1,))) for par in (0, 1)]
        return s, dp

    products = [block_products(0)]

    for o in range(1, n):
        id_copy(o).wait_send()
        remote(ids, idbuf.at[lax.rem(d - o + n, n)], id_s.at[o - 1], id_r.at[o - 1],
               ctx=lax.rem(d + o, n)).wait_recv()
    for k in range(1, reach):
        @pl.when(d - k >= 0)
        def _(k=k):
            key_copy(k).wait_recv()
    for k in range(1, reach):
        products.append(block_products(k))

    allowed = []
    for k in range(reach):
        r = rows_of[k]
        row = own_ids if k == 0 else idbuf[jnp.maximum(d - k, 0)]
        row = row[:, tok - r:]
        lane = lax.broadcasted_iota(jnp.int32, (1, r), 1)
        ok = qid == row
        if k == 0:
            ok = ok & (lane <= tok - qd + qrow)
        else:
            reachable = jnp.where(lane + (tok - r) >= (k + 1) * tok - span, 1, 0)
            reachable = reachable * jnp.where(d - k >= 0, 1, 0)
            ok = ok & (reachable == 1)
        allowed.append(ok)

    dscores, probs = [[], []], [[], []]
    for par in (0, 1):
        s = [jnp.where(allowed[k], products[k][0][par] * score_scale, -1e30) for k in range(reach)]
        top = functools.reduce(jnp.maximum, [jnp.max(x, axis=1, keepdims=True) for x in s])
        w = [jnp.exp(x - top) for x in s]
        total = sum(jnp.sum(x, axis=1, keepdims=True) for x in w)
        w = [x / total for x in w]
        dps = [products[k][1][par] for k in range(reach)]
        rd = sum(jnp.sum(a * b, axis=1, keepdims=True) for a, b in zip(w, dps))
        for k in range(reach):
            dscores[par].append((w[k] * (dps[k] - rd) * score_scale).astype(BF))
            probs[par].append(w[k].astype(BF))

    def part_of(k):
        a = dot(dscores[0][k], query(0), ((0,), (0,)))[:, :kw]
        b = dot(dscores[1][k], query(1), ((0,), (0,)))[:, pad:pad + kw]
        v = dot(probs[0][k], grad(0), ((0,), (0,))) + dot(probs[1][k], grad(1), ((0,), (0,)))
        return (a + b + jnp.concatenate([v, jnp.zeros((rows_of[k], kw - LATENT), F32)], axis=1)).astype(BF)

    def part_copy(k, to):
        r = rows_of[k]
        return remote(psend.at[k - 1, pl.ds(0, r)], precv.at[k - 1, pl.ds(0, r)],
                      part_s.at[k - 1], part_r.at[k - 1], ctx=to)

    for k in range(1, reach):
        psend[k - 1, 0:rows_of[k], :] = part_of(k)

        @pl.when(d - k >= 0)
        def _(k=k):
            part_copy(k, jnp.maximum(d - k, 0)).start()

        @pl.when(d + k >= n)
        def _(k=k):
            precv[k - 1] = jnp.zeros_like(precv[k - 1])
    mine = part_of(0).astype(F32)

    eye = lax.broadcasted_iota(jnp.int32, (tok, tok), 0) == lax.broadcasted_iota(jnp.int32, (tok, tok), 1)
    doc_lane = lax.broadcasted_iota(jnp.int32, (1, 128), 1)
    member = []
    for j in range(n):
        col = jnp.sum(jnp.where(eye, idbuf[j], 0).astype(F32), axis=1, keepdims=True)
        member.append(jnp.where(col == doc_lane.astype(F32), 1.0, 0.0))

    for k in range(1, reach):
        @pl.when(d + k < n)
        def _(k=k):
            part_copy(k, jnp.maximum(d - k, 0)).wait_recv()
    for k in range(1, reach):
        r = rows_of[k]
        got = precv[k - 1, 0:r, :].astype(F32)
        if r < tok:
            got = jnp.concatenate([jnp.zeros((tok - r, kw), F32), got], axis=0)
        mine = mine + got
    mine_low = mine.astype(BF)
    full[d] = mine_low

    piece = tok // pieces

    def relay(direction, s, p):
        ss, rs = (up_s, up_r) if direction > 0 else (dn_s, dn_r)
        block = jnp.clip(d - direction * s, 0, n - 1)
        ref = full.at[block, pl.ds(p * piece, piece)]
        return remote(ref, ref, ss.at[s, p], rs.at[s, p], ctx=jnp.clip(d + direction, 0, n - 1))

    def arriving(direction, s, p):
        ss, rs = (up_s, up_r) if direction > 0 else (dn_s, dn_r)
        block = jnp.clip(d - direction * (s + 1), 0, n - 1)
        ref = full.at[block, pl.ds(p * piece, piece)]
        return remote(ref, ref, ss.at[s, p], rs.at[s, p], ctx=jnp.clip(d + direction, 0, n - 1))

    def can_send(direction, s):
        if direction > 0:
            return (d - s >= 0) & (d + 1 < n)
        return (d + s < n) & (d - 1 >= 0)

    def will_get(direction, s):
        return d - s - 1 >= 0 if direction > 0 else d + s + 1 < n

    for p in range(pieces):
        for direction in (1, -1):
            @pl.when(can_send(direction, 0))
            def _(p=p, direction=direction):
                relay(direction, 0, p).start()
    padded_out = jnp.concatenate([mine_low.astype(F32), jnp.zeros((tok, pad), F32)], axis=1)
    gk_out[0] = jnp.transpose(padded_out)[:kw].astype(BF)
    for s in range(n - 1):
        for p in range(pieces):
            for direction in (1, -1):
                @pl.when(will_get(direction, s))
                def _(p=p, s=s, direction=direction):
                    arriving(direction, s, p).wait_recv()
                if s + 1 < n - 1:
                    @pl.when(can_send(direction, s + 1))
                    def _(p=p, s=s, direction=direction):
                        relay(direction, s + 1, p).start()

    norms = jnp.zeros((1, 128), F32)
    for j in range(n):
        v = full[j].astype(F32)
        norms = norms + jnp.sum(member[j] * jnp.sum(v * v, axis=1, keepdims=True), axis=0, keepdims=True)
    limits = lim[...]
    if ndocs < 128:
        limits = jnp.concatenate([limits, jnp.zeros((1, 128 - ndocs), F32)], axis=1)
    factor = jnp.minimum(1.0, limits / jnp.sqrt(norms + norm_eps))
    for j in range(n):
        f = jnp.sum(member[j] * factor, axis=1, keepdims=True)
        scaled = (full[j].astype(F32) * f).astype(BF).astype(F32)
        scaled = jnp.concatenate([scaled, jnp.zeros((tok, pad), F32)], axis=1)
        turned = jnp.transpose(scaled)
        scT[:, j * tok:(j + 1) * tok] = turned[:kw].astype(BF)

    copy_h.wait()
    w_out[...] = dot(scT[...], hid[0], ((1,), (0,)))

    for k in range(1, reach):
        @pl.when(d + k < n)
        def _(k=k):
            key_copy(k).wait_send()

        @pl.when(d - k >= 0)
        def _(k=k):
            part_copy(k, jnp.maximum(d - k, 0)).wait_send()
    for s in range(n - 1):
        for p in range(pieces):
            for direction in (1, -1):
                @pl.when(can_send(direction, s))
                def _(p=p, s=s, direction=direction):
                    relay(direction, s, p).wait_send()


def flush(gk, w, gk_out, w_out, sem):
    a = pltpu.make_async_copy(gk, gk_out, sem.at[0])
    b = pltpu.make_async_copy(w, w_out, sem.at[1])
    a.start()
    b.start()
    a.wait()
    b.wait()


def pair_body(cfg, *refs):
    n = cfg["n"]
    tok = cfg["tok"]
    kw = cfg["kw"]
    qd = cfg["qd"]
    halo = cfg["halo"]
    ndocs = cfg["ndocs"]
    splits = cfg["splits"]
    seq = n * tok
    wide = -(-kw // 128) * 128
    pad = wide - kw
    share = kw // 8
    np_ = len(splits)
    offs = [sum(splits[:p]) for p in range(np_)]
    (lat_hbm, ids_hbm, lim_hbm, q_hbm, g_hbm, h_hbm, gk_dst, w_dst,
     gk_out, w_out, lat_t, lat, ids, lim, qraw, graw, hid, qs, gs, kbuf, krot, kgot, lath, hkey, idbuf,
     psend, precv, hsend, hrecv, ownb, own2, full, gkr, nbuf, lhs,
     loc, out_s, key_r, hid_r, part_r, halo_r, own_r, gk_r, nrm_r, blk_r, rs_r) = refs[:46]
    tail = refs[46:]
    d = lax.axis_index("ctx")
    m = lax.axis_index("grp")
    c = lax.rem(m, 2)
    xb = lax.rem(m // 2, 2)
    yb = lax.rem(m // 4, 2)
    base = m - c
    mate = base + 1 - c
    flip_x = m + 2 - 4 * xb
    flip_y = m + 4 - 8 * yb
    flip_xy = flip_x + flip_y - m
    cols = w_out.shape[1]
    wing = cols // 2

    def remote(src, dst, ss, rs, **where):
        return pltpu.make_async_remote_copy(
            src_ref=src, dst_ref=dst, send_sem=ss, recv_sem=rs,
            device_id=where, device_id_type=pl.DeviceIdType.MESH,
        )

    def drain(ref, sem):
        pltpu.make_async_copy(ref, ref, sem).wait()

    loads = [
        pltpu.make_async_copy(lat_hbm, lat_t, loc.at[0]),
        pltpu.make_async_copy(ids_hbm, ids, loc.at[1]),
        pltpu.make_async_copy(q_hbm, qraw, loc.at[2]),
        pltpu.make_async_copy(g_hbm, graw, loc.at[3]),
        pltpu.make_async_copy(lim_hbm, lim, loc.at[4]),
        pltpu.make_async_copy(h_hbm.at[0], hid.at[c], loc.at[5]),
    ]
    for copy in loads:
        copy.start()

    barrier = pltpu.get_barrier_semaphore()

    def greet(**where):
        pl.semaphore_signal(barrier, inc=1, device_id=where, device_id_type=pl.DeviceIdType.MESH)

    close = 0
    for o in (-2, 2, -1, 1):
        there = (d + o >= 0) & (d + o < n)
        close = close + jnp.where(there, 2, 0)

        @pl.when(there)
        def _(o=o):
            for who in (m, mate):
                greet(ctx=jnp.clip(d + o, 0, n - 1), grp=who)
    greet(grp=mate)
    greet(grp=flip_x)
    greet(grp=flip_y)
    greet(grp=flip_xy)

    loads[0].wait()
    keys_t = jnp.concatenate([lat_t[0].astype(F32), jnp.zeros((pad, tok), F32)], axis=0)
    keys = jnp.transpose(keys_t)
    lat[...] = keys.astype(BF)
    near = tok // 2
    rope = kw - LATENT
    krot[...] = jnp.concatenate([keys[:near, LATENT:kw], keys[near:, LATENT:kw]], axis=1).astype(BF)
    lath[...] = keys[tok - halo:].astype(BF)
    loads[1].wait()
    pl.semaphore_wait(barrier, close + 4)

    def id_copy(k):
        return remote(ids, idbuf.at[k - 1], out_s.at[12 + k], key_r.at[k - 1], ctx=lax.rem(d + k, n))

    def key_copy(k):
        if k == 1:
            return [
                remote(lat.at[:, pl.ds(0, LATENT)], kbuf.at[pl.ds(0, tok), pl.ds(0, LATENT)],
                       out_s.at[15], key_r.at[2], ctx=lax.rem(d + 1, n)),
                remote(krot, kgot, out_s.at[16], key_r.at[3], ctx=lax.rem(d + 1, n)),
            ]
        return [remote(lath, hkey, out_s.at[17], key_r.at[4], ctx=lax.rem(d + 2, n))]

    for k in (2, 1):
        @pl.when(d + k < n)
        def _(k=k):
            id_copy(k).start()
            for copy in key_copy(k):
                copy.start()

    hid_copy = remote(h_hbm.at[0], hid.at[c], out_s.at[0], hid_r.at[0], grp=mate)
    hid_copy.start()

    @pl.when(d < 1)
    def _():
        kbuf[0:tok, :] = jnp.zeros((tok, wide), BF)
        kgot[...] = jnp.zeros_like(kgot)
        idbuf[0] = jnp.zeros_like(idbuf[0])

    @pl.when(d < 2)
    def _():
        hkey[...] = jnp.zeros_like(hkey)
        idbuf[1] = jnp.zeros_like(idbuf[1])

    group = 16 // qd
    R = (HEADS // 2) * qd

    def repack(src, dst, width):
        def step(i, _):
            got = [
                src[0, :, pl.ds(pl.multiple_of((i * group + t) * 2 * width, 128), 2 * width)].astype(F32)
                for t in range(group)
            ]
            got = jnp.concatenate(got, axis=0)
            for par in (0, 1):
                one = got[:, par * width:(par + 1) * width]
                if width % 128:
                    one = jnp.concatenate([one, jnp.zeros((16, pad), F32)], axis=1)
                dst[pl.ds(pl.multiple_of(par * R + i * 16, 16), 16), :] = one.astype(BF)
            return 0

        lax.fori_loop(0, (HEADS // 2) // group, step, 0)

    loads[2].wait()
    repack(qraw, qs, kw)
    loads[3].wait()
    repack(graw, gs, LATENT)

    def turn_ids(row):
        return jnp.transpose(jnp.broadcast_to(row.astype(F32), (tok, tok)))

    def across(x):
        return jnp.concatenate([x] * (2 * R // tok), axis=1)

    qrow = lax.broadcasted_iota(jnp.int32, (1, tok), 1) % qd
    own_ids = ids[...]
    qid = jnp.zeros((1, tok), F32)
    for i in range(qd):
        qid = jnp.where(qrow == i, own_ids[:, tok - qd + i:tok - qd + i + 1].astype(F32), qid)

    def block_products(keys):
        return (dot(keys, qs[...], ((1,), (1,))), dot(keys[:, :LATENT], gs[...], ((1,), (1,))))

    key_row = lax.broadcasted_iota(jnp.int32, (tok, tok), 0)
    s0, dp0 = block_products(lat[...])
    ok0 = jnp.where(turn_ids(own_ids) == qid, 1, 0) * jnp.where(key_row <= tok - qd + qrow, 1, 0)
    s0 = jnp.where(across(ok0) == 1, s0 * score_scale, -1e30)
    top0 = jnp.max(s0, axis=0, keepdims=True)

    for k in (2, 1):
        @pl.when(d >= k)
        def _(k=k):
            id_copy(k).wait_recv()
            for copy in key_copy(k):
                copy.wait_recv()
    got = kgot[...].astype(F32)
    got = jnp.concatenate([got[:, :rope], got[:, rope:]], axis=0)
    kbuf[0:tok, LATENT:wide] = jnp.concatenate([got, jnp.zeros((tok, wide - kw), F32)], axis=1).astype(BF)
    kbuf[tok:tok + 16, :] = jnp.concatenate([jnp.zeros((16 - halo, wide), F32), hkey[...].astype(F32)], axis=0).astype(BF)
    s1, dp1 = block_products(kbuf[...])
    ok1 = jnp.where(turn_ids(idbuf[0]) == qid, 1, 0)
    ok1 = ok1 * jnp.where(key_row >= 2 * tok - cfg["span"], 1, 0) * jnp.where(d >= 1, 1, 0)
    ok2 = jnp.where(turn_ids(idbuf[1]) == qid, 1, 0)
    ok2 = ok2 * jnp.where(key_row >= 3 * tok - cfg["span"], 1, 0) * jnp.where(d >= 2, 1, 0)
    ok1 = jnp.concatenate([ok1, ok2[tok - 16:]], axis=0)
    s1 = jnp.where(across(ok1) == 1, s1 * score_scale, -1e30)
    top = jnp.maximum(top0, jnp.max(s1, axis=0, keepdims=True))
    w0, w1 = jnp.exp(s0 - top), jnp.exp(s1 - top)
    scale = 1.0 / (jnp.sum(w0, axis=0, keepdims=True) + jnp.sum(w1, axis=0, keepdims=True))
    w0, w1 = w0 * scale, w1 * scale
    rd = jnp.sum(w0 * dp0, axis=0, keepdims=True) + jnp.sum(w1 * dp1, axis=0, keepdims=True)

    def part_of(w, dp):
        a = dot((w * (dp - rd) * score_scale).astype(BF), qs[...], ((1,), (0,)))
        v = dot(w.astype(BF), gs[...], ((1,), (0,)))
        return a + jnp.concatenate([v, jnp.zeros((v.shape[0], wide - LATENT), F32)], axis=1)

    def halves(turned):
        out = []
        for h in (0, 1):
            rows = []
            for p in range(np_):
                for q in range(4):
                    start = share * (2 * q + h) + offs[p]
                    rows.append(turned[start:start + splits[p]])
            out.append(jnp.concatenate(rows, axis=0))
        return out

    def halo_copy(h):
        return remote(hsend, hrecv.at[c], out_s.at[2], halo_r.at[0],
                      ctx=jnp.maximum(d - 2, 0), grp=base + h)

    def part_copy(h, p):
        rows = pl.ds(4 * offs[p], 4 * splits[p])
        return remote(psend.at[h, rows], precv.at[c, rows], out_s.at[1], part_r.at[p],
                      ctx=jnp.maximum(d - 1, 0), grp=base + h)

    part1 = part_of(w1, dp1)
    hsend[...] = part1[tok + 16 - halo:].astype(BF)

    @pl.when(d >= 2)
    def _():
        for h in (0, 1):
            halo_copy(h).start()

    turned = halves(jnp.transpose(part1[:tok]))
    for h in (0, 1):
        psend[h] = turned[h].astype(BF)

    @pl.when(d >= 1)
    def _():
        for p in range(np_):
            for h in (0, 1):
                part_copy(h, p).start()

    @pl.when(d + 1 >= n)
    def _():
        precv[...] = jnp.zeros_like(precv)

    @pl.when(d + 2 >= n)
    def _():
        hrecv[...] = jnp.zeros_like(hrecv)

    turned = halves(jnp.transpose(part_of(w0, dp0)))
    for h in (0, 1):
        ownb[h] = turned[h].astype(BF)
    own_copy = remote(ownb.at[1 - c], own2.at[c], out_s.at[3], own_r.at[0], grp=mate)
    own_copy.start()
    own2[c] = ownb[c]
    own_copy.wait_recv()

    def rows_at(p):
        return pl.ds(8 * offs[p], 8 * splits[p])

    steps = (-1, 1, -2, 2)

    def slot(o, source):
        if o in (-1, 1):
            return 1
        return jnp.where(source == (n - 1 if o < 0 else 0), 0, 1)

    def spread(o, p):
        ref = full.at[d, rows_at(p)]
        return remote(ref, ref, out_s.at[7 + steps.index(o)], blk_r.at[slot(o, d), p], ctx=jnp.clip(d + o, 0, n - 1))

    def spread_from(o, p):
        ref = full.at[jnp.clip(d - o, 0, n - 1), rows_at(p)]
        return remote(ref, ref, out_s.at[7 + steps.index(o)], blk_r.at[slot(o, d - o), p], ctx=jnp.clip(d - o, 0, n - 1))

    def pass_end(o, p):
        ref = full.at[n - 1 if o < 0 else 0, rows_at(p)]
        return remote(ref, ref, out_s.at[11 if o < 0 else 12], blk_r.at[1, p], ctx=jnp.clip(d + o, 0, n - 1))

    def reaches(o):
        return (d + o >= 0) & (d + o < n)

    def passes(o):
        return d == (1 if o < 0 else n - 2)

    def ends(o):
        return d == (0 if o < 0 else n - 1)

    @pl.when(d + 2 < n)
    def _():
        drain(hrecv, halo_r.at[0])

    side = []
    for g in (0, 1):
        block = jnp.concatenate([jnp.zeros((tok - halo, wide), F32), hrecv[g].astype(F32)], axis=0)
        turned = halves(jnp.transpose(block))
        side.append(jnp.where(c == 0, turned[0], turned[1]))

    def spread_all(p):
        for o in steps:
            @pl.when(reaches(o))
            def _(o=o):
                spread(o, p).start()

    token_norm = [jnp.zeros((1, tok), F32) for _ in (0, 1)]
    for p in range(np_):
        @pl.when(d + 1 < n)
        def _(p=p):
            drain(precv.at[:, pl.ds(4 * offs[p], 4 * splits[p])], part_r.at[p])
        lo, size = 4 * offs[p], 4 * splits[p]
        for g in (0, 1):
            value = own2[g, lo:lo + size].astype(F32) + precv[g, lo:lo + size].astype(F32)
            value = (value + side[g][lo:lo + size]).astype(BF)
            full[d, 2 * lo + g * size:2 * lo + (g + 1) * size] = value
            value = value.astype(F32)
            token_norm[g] = token_norm[g] + jnp.sum(value * value, axis=0, keepdims=True)
        if p == 0:
            spread_all(p)

    loads[4].wait()
    limits = jnp.concatenate([lim[...], jnp.zeros((1, tok - ndocs), F32)], axis=1)
    nbuf[c, d] = jnp.concatenate(
        token_norm + [own_ids.astype(F32), limits, jnp.zeros((4, tok), F32)], axis=0)

    def norm_copy(o, flip):
        ref = nbuf.at[c, d]
        return remote(ref, ref, out_s.at[5 + flip], nrm_r.at[flip], ctx=lax.rem(d + o, n), grp=mate if flip else m)

    peers = [(o, flip) for o in range(n) for flip in (0, 1) if o or flip]
    for o, flip in peers:
        norm_copy(o, flip).start()
    spread_all(1)

    def spread_rest(p):
        if p < np_:
            @pl.when(ends(-1) | ends(1))
            def _():
                spread_all(p)

    def spread_mid(p):
        if p < np_:
            @pl.when(jnp.logical_not(ends(-1) | ends(1)))
            def _():
                spread_all(p)

    for p in range(2, np_):
        spread_rest(p)

    def gk_copy(p):
        lo, size = 4 * offs[p], 4 * splits[p]
        src = full.at[d, pl.ds(pl.multiple_of(2 * lo + (1 - c) * size, 16), size)]
        return remote(src, gkr.at[pl.ds(lo, size)], out_s.at[4], gk_r.at[0], grp=mate)

    for p in range(np_):
        gk_copy(p).start()

    factors = []

    def make_factors():
        drain(nbuf.at[0, pl.ds(0, n - 1)], nrm_r.at[0])
        drain(nbuf.at[0], nrm_r.at[1])
        rows = -(-ndocs // 8) * 8
        sub = lax.broadcasted_iota(jnp.int32, (rows, tok), 0).astype(F32)
        lane = lax.broadcasted_iota(jnp.int32, (rows, tok), 1).astype(F32)
        for g in (0, 1):
            member = [jnp.where(nbuf[g, b, 2:3] == sub, 1.0, 0.0) for b in range(n)]
            norms = sum(
                jnp.sum(member[b] * (nbuf[0, b, g:g + 1] + nbuf[1, b, g:g + 1]), axis=1, keepdims=True)
                for b in range(n))
            top = jnp.sum(jnp.where(lane == sub, nbuf[g, 0, 3:4], 0.0), axis=1, keepdims=True)
            factor = jnp.minimum(1.0, top / jnp.sqrt(norms + norm_eps))
            factors.append([jnp.sum(member[b] * factor, axis=0, keepdims=True) for b in range(n)])

    def forward(p):
        for o in (-1, 1):
            @pl.when(passes(o))
            def _(o=o):
                spread_from(2 * o, p).wait_recv()
                pass_end(o, p).start()
        spread_mid(p + 2)

    def gather(p):
        @pl.when(ends(-1) | ends(1))
        def _():
            drain(full.at[pl.ds(0, n - 1), rows_at(p)], blk_r.at[1, p])

        @pl.when(jnp.logical_not(ends(-1) | ends(1)))
        def _():
            drain(full.at[pl.ds(0, n - 2), rows_at(p)], blk_r.at[1, p])

    straight = cfg["straight"]
    bufs, pos = [], 0
    for p in range(np_):
        if p in straight:
            bufs.append(tail[pos:pos + 3])
            pos += 3
        else:
            bufs.append(tail[pos:pos + 3])
            pos += 3

    def direct(p, j):
        out, back, _ = bufs[p]
        return remote(out.at[j], back.at[j], out_s.at[18 + p], rs_r.at[p, 0, 0],
                      grp=(flip_x, flip_y, flip_xy)[j])

    def hop(p, w, stage):
        out, back, _ = bufs[p]
        where = (flip_x, flip_y) if w == 0 else (flip_y, flip_x)
        part = pl.ds(0, 2) if stage == 0 else pl.ds(2, 1)
        src, dst = out.at[w, part], back.at[w, part]
        return remote(src, dst, out_s.at[18 + p], rs_r.at[p, w, stage], grp=where[stage])

    bits = ((xb, yb), (yb, xb))

    def chip(w, moving, other):
        return other * 2 + moving if w == 0 else moving * 2 + other

    def wing_of(p, w):
        lo, size = 4 * offs[p], 4 * splits[p]
        return sum(
            dot(lhs[lo:lo + size, g * seq:(g + 1) * seq], hid[g, :, w * wing:(w + 1) * wing], ((1,), (0,)))
            for g in (0, 1))

    def product(p):
        lo, size = 4 * offs[p], 4 * splits[p]
        for g in (0, 1):
            for b in range(n):
                value = full[b, 2 * lo + g * size:2 * lo + (g + 1) * size].astype(F32)
                at = (g * n + b) * tok
                lhs[lo:lo + size, at:at + tok] = (value * factors[g][b]).astype(BF)
        if p in straight:
            first, _, total = bufs[p]
            for w in (0, 1):
                cut = slice(w * wing, (w + 1) * wing)
                total[:, :, cut] = wing_of(p, w).reshape(4, splits[p], wing)
            for j, q in ((2, 2 * (1 - yb) + 1 - xb), (0, 2 * yb + 1 - xb), (1, 2 * (1 - yb) + xb)):
                first[j] = total[q].astype(BF)
                direct(p, j).start()
            return
        for w in (0, 1):
            first, _, total = bufs[p]
            total[w] = wing_of(p, w).reshape(total.shape[1:])
            for o in (0, 1):
                first[w, o] = total[w, chip(w, 1 - bits[w][0], o)].astype(BF)
            hop(p, w, 0).start()

    def pass_on(p):
        for w in (0, 1):
            second, back, total = bufs[p]
            hop(p, w, 0).wait_recv()
            second[w, 2] = (total[w, chip(w, bits[w][0], 1 - bits[w][1])] + back[w, 1 - bits[w][1]].astype(F32)).astype(BF)
            hop(p, w, 1).start()

    def put(p):
        rows = pl.ds(offs[p], splits[p])
        return pltpu.make_async_copy(w_out.at[rows], w_dst.at[rows], loc.at[7])

    put_keys = pltpu.make_async_copy(gk_out, gk_dst, loc.at[6])

    def finish(p):
        last(p)
        put(p).start()

    def last(p):
        if p in straight:
            _, back, total = bufs[p]
            value = total[2 * yb + xb]
            drain(back, rs_r.at[p, 0, 0])
            for j in range(3):
                value = value + back[j].astype(F32)
            w_out[offs[p]:offs[p] + splits[p], :] = value
            return
        for w in (0, 1):
            _, back, total = bufs[p]
            kept = total[w, chip(w, bits[w][0], bits[w][1])] + back[w, bits[w][1]].astype(F32)
            hop(p, w, 1).wait_recv()
            w_out[offs[p]:offs[p] + splits[p], w * wing:(w + 1) * wing] = kept + back[w, 2].astype(F32)

    def write_keys():
        drain(gkr, gk_r.at[0])
        order = [None] * (8 * np_)
        for p in range(np_):
            lo, size = 4 * offs[p], splits[p]
            near = [full[d, 2 * lo + g * 4 * size:2 * lo + (g + 1) * 4 * size].astype(F32) for g in (0, 1)]
            near = jnp.where(c == 0, near[0], near[1])
            far = gkr[lo:lo + 4 * size].astype(F32)
            for h in (0, 1):
                value = jnp.where(c == h, near, far)
                for q in range(4):
                    order[(2 * q + h) * np_ + p] = value[q * size:(q + 1) * size]
        gk_out[0] = jnp.concatenate(order, axis=0).astype(BF)
        put_keys.start()

    forward(0)
    make_factors()
    loads[5].wait()
    hid_copy.wait_recv()
    staged = [p for p in range(np_) if p not in straight]
    moved, done = [], []
    for p in range(np_):
        if p + 1 < np_:
            forward(p + 1)
        gather(p)
        product(p)
        if p == 0:
            write_keys()
        for q in staged:
            if q + cfg["lag"] == p:
                pass_on(q)
                moved.append(q)
            if q + 2 * cfg["lag"] == p:
                finish(q)
                done.append(q)
    for q in staged:
        if q not in moved:
            pass_on(q)
    for q in range(np_):
        if q not in done:
            finish(q)
    put_keys.wait()
    drain(w_out, loc.at[7])

    for k in (1, 2):
        @pl.when(d + k < n)
        def _(k=k):
            id_copy(k).wait_send()
            for copy in key_copy(k):
                copy.wait_send()
    hid_copy.wait_send()

    @pl.when(d >= 2)
    def _():
        drain(hrecv, out_s.at[2])

    @pl.when(d >= 1)
    def _():
        drain(psend, out_s.at[1])
    own_copy.wait_send()
    drain(gkr, out_s.at[4])
    drain(nbuf.at[0, pl.ds(0, n - 1)], out_s.at[5])
    drain(nbuf.at[0], out_s.at[6])
    for i, o in enumerate(steps):
        @pl.when(reaches(o))
        def _(i=i):
            drain(full.at[0], out_s.at[7 + i])
    for i, o in enumerate((-1, 1)):
        @pl.when(passes(o))
        def _(i=i):
            drain(full.at[0], out_s.at[11 + i])
    for p in range(np_):
        drain(bufs[p][0], out_s.at[18 + p])


def pair_scratch(cfg, latent, queries, out_grad, hidden, clip_limits):
    n, tok, kw, halo = cfg["n"], cfg["tok"], cfg["kw"], cfg["halo"]
    splits = cfg["splits"]
    np_ = len(splits)
    half = kw // 2
    wide = -(-kw // 128) * 128
    rows = (HEADS // 2) * cfg["qd"]
    cols = hidden.shape[2]
    seq = n * tok
    dma = pltpu.SemaphoreType.DMA
    v = pltpu.VMEM
    scratch = [
        v((1, kw, tok), BF), v((kw // 8, cols), F32),
        v((1, kw, tok), BF), v((tok, wide), BF), v((1, tok), jnp.int32), v(clip_limits.shape, F32),
        v(queries.shape, BF), v(out_grad.shape, BF), v((2, seq, cols), BF),
        v((2 * rows, wide), BF), v((2 * rows, LATENT), BF),
        v((tok + 16, wide), BF), v((tok // 2, 2 * (kw - LATENT)), BF), v((tok // 2, 2 * (kw - LATENT)), BF),
        v((halo, wide), BF), v((halo, wide), BF), v((2, 1, tok), jnp.int32),
        v((2, half, tok), BF), v((2, half, tok), BF), v((halo, wide), BF), v((2, halo, wide), BF),
        v((2, half, tok), BF), v((2, half, tok), BF), v((n, kw, tok), BF), v((half, tok), BF),
        v((2, n, 8, tok), F32), v((half, 2 * seq), BF),
        dma((8,)), dma((18 + np_,)), dma((5,)), dma((1,)), dma((np_,)), dma((1,)), dma((1,)), dma((1,)), dma((2,)),
        dma((2, np_)), dma((np_, 2, 2)),
    ]
    for p, size in enumerate(splits):
        if p in cfg["straight"]:
            scratch += [v((3, size, cols), BF), v((3, size, cols), BF), v((4, size, cols), F32)]
            continue
        scratch += [
            v((2, 3, size, cols // 2), BF), v((2, 3, size, cols // 2), BF), v((2, 4, size, cols // 2), F32),
        ]
    return scratch


def row_splits(share):
    units = share // 8
    cuts = [0] + [units * p // 9 for p in (3, 6)] + [units]
    return tuple(8 * (b - a) for a, b in zip(cuts, cuts[1:]) if b > a)


def pair_call(cfg, latent, queries, out_grad, hidden, doc_ids, clip_limits):
    anywhere = pl.BlockSpec(memory_space=pl.ANY)
    tok, kw = cfg["tok"], cfg["kw"]
    grad_keys, weight = pl.pallas_call(
        functools.partial(pair_body, cfg),
        out_shape=(
            pltpu.VMEM((1, kw, tok), BF),
            pltpu.VMEM((kw // 8, hidden.shape[2]), F32),
        ),
        in_specs=[anywhere] * 6,
        out_specs=(anywhere, anywhere),
        scratch_shapes=pair_scratch(cfg, latent, queries, out_grad, hidden, clip_limits),
        compiler_params=pltpu.CompilerParams(
            collective_id=0, has_side_effects=True, vmem_limit_bytes=56 * 1024 * 1024),
    )(jnp.swapaxes(latent, 1, 2), doc_ids, clip_limits, queries, out_grad, hidden)
    return (jnp.swapaxes(grad_keys, 1, 2), weight)


def on_device(latent, queries, out_grad, hidden, doc_ids, clip_limits):
    n = lax.axis_size("ctx")
    groups = lax.axis_size("grp")
    tok, kw = latent.shape[1:]
    qd = queries.shape[1]
    seq = tok * n
    span = seq // 2 + qd
    reach = min(n, -(-span // tok))
    cols = hidden.shape[2]
    last = min(tok, -(-(span - (reach - 1) * tok) // 16) * 16)
    rows_of = [tok] * (reach - 1) + [last]
    ndocs = clip_limits.shape[1]
    share = kw // 8
    paired = (groups == 8 and n == 4 and reach == 3 and last <= tok and cols % 256 == 0 and kw % 64 == 0
              and tok % 128 == 0 and ndocs <= tok and span <= 2 * tok + 16 and 2 * (kw - LATENT) == 128)
    if paired:
        cfg = dict(n=n, tok=tok, kw=kw, qd=qd, halo=-(-(span - 2 * tok) // 4) * 4, span=span, ndocs=ndocs, splits=row_splits(share), straight=(0,), lag=1)
        return pair_call(cfg, latent, queries, out_grad, hidden, doc_ids, clip_limits)
    pieces = 2
    cfg = dict(n=n, tok=tok, kw=kw, qd=qd, reach=reach, rows_of=rows_of, span=span, ndocs=ndocs,
               pieces=pieces)
    rows = (HEADS // 2) * qd
    dma = pltpu.SemaphoreType.DMA
    scratch = [
        pltpu.VMEM(queries.shape, BF),
        pltpu.VMEM(out_grad.shape, BF),
        pltpu.VMEM(hidden.shape, BF),
        pltpu.VMEM((rows, 2 * kw), BF),
        pltpu.VMEM((rows, 2 * LATENT), BF),
        pltpu.VMEM((reach - 1, tok, kw), BF),
        pltpu.VMEM((n, 1, tok), jnp.int32),
        pltpu.VMEM((reach - 1, tok, kw), BF),
        pltpu.VMEM((reach - 1, tok, kw), BF),
        pltpu.VMEM((n, tok, kw), BF),
        pltpu.VMEM((kw, seq), BF),
        dma((3,)),
        dma((reach - 1,)), dma((reach - 1,)),
        dma((n - 1,)), dma((n - 1,)),
        dma((reach - 1,)), dma((reach - 1,)),
        dma((n - 1, pieces)), dma((n - 1, pieces)),
        dma((n - 1, pieces)), dma((n - 1, pieces)),
        pltpu.VMEM((1, tok, kw), BF),
    ]
    vmem = pl.BlockSpec(memory_space=pltpu.VMEM)
    anywhere = pl.BlockSpec(memory_space=pl.ANY)
    grad_keys, weight = pl.pallas_call(
        functools.partial(body, cfg),
        out_shape=(
            jax.ShapeDtypeStruct((1, kw, tok), BF),
            jax.ShapeDtypeStruct((kw, cols), F32),
        ),
        in_specs=[vmem, vmem, vmem, anywhere, anywhere, anywhere],
        out_specs=(vmem, vmem),
        scratch_shapes=scratch,
        compiler_params=pltpu.CompilerParams(
            collective_id=0, has_side_effects=True, vmem_limit_bytes=60 * 1024 * 1024),
    )(jnp.swapaxes(latent, 1, 2), doc_ids, clip_limits, queries, out_grad, hidden)
    weight = lax.psum_scatter(weight, "grp", scatter_dimension=0, tiled=True)
    return (jnp.swapaxes(grad_keys, 1, 2), weight)


def solution(mesh):
    return jax.shard_map(
        on_device,
        mesh=mesh,
        in_specs=(
            P("grp", "ctx", None),
            P("grp", "ctx", None),
            P("grp", "ctx", None),
            P("grp", None, "ctx"),
            P("grp", "ctx"),
            P("grp", None),
        ),
        out_specs=(P("grp", "ctx", None), P("grp", "ctx")),
        check_vma=False,
    )
```

```python
import functools
import math

import jax
import jax.numpy as jnp
from jax import lax
from jax.experimental import pallas as pl
from jax.experimental.pallas import tpu as pltpu
from jax.sharding import PartitionSpec as P

LATENT = 512
HEADS = 128


score_scale = 192.0 ** (-0.5)
norm_eps = 1e-06

BF = jnp.bfloat16
F32 = jnp.float32


def dot(a, b, dims):
    return lax.dot_general(a, b, (dims, ((), ())), preferred_element_type=F32)


def body(cfg, *refs):
    n = cfg["n"]
    tok = cfg["tok"]
    kw = cfg["kw"]
    qd = cfg["qd"]
    reach = cfg["reach"]
    rows_of = cfg["rows_of"]
    span = cfg["span"]
    ndocs = cfg["ndocs"]
    pieces = cfg["pieces"]
    (lat_t, ids, lim, q_hbm, g_hbm, h_hbm, gk_out, w_out) = refs[:8]
    (qraw, graw, hid, qs, gs, kbuf, idbuf, psend, precv, full, scT, local_sem, key_s, key_r,
     id_s, id_r, part_s, part_r, up_s, up_r, dn_s, dn_r, lat) = refs[8:31]
    d = lax.axis_index("ctx")
    wide = -(-kw // 128) * 128
    pad = wide - kw
    pair = 2 * kw

    copy_q = pltpu.make_async_copy(q_hbm, qraw, local_sem.at[0])
    copy_g = pltpu.make_async_copy(g_hbm, graw, local_sem.at[1])
    copy_h = pltpu.make_async_copy(h_hbm, hid, local_sem.at[2])
    copy_q.start()
    copy_g.start()
    copy_h.start()

    def remote(src, dst, ss, rs, **where):
        axis, index = next(iter(where.items()))
        return pltpu.make_async_remote_copy(
            src_ref=src, dst_ref=dst, send_sem=ss, recv_sem=rs,
            device_id={axis: index}, device_id_type=pl.DeviceIdType.MESH,
        )

    barrier = pltpu.get_barrier_semaphore()
    for o in range(1, n):
        pl.semaphore_signal(barrier, inc=1, device_id={"ctx": lax.rem(d + o, n)},
                            device_id_type=pl.DeviceIdType.MESH)
    keys_t = jnp.concatenate([lat_t[0].astype(F32), jnp.zeros((pad, tok), F32)], axis=0)
    lat[0] = jnp.transpose(keys_t)[:, :kw].astype(BF)
    pl.semaphore_wait(barrier, n - 1)

    def key_copy(k):
        r = rows_of[k]
        return remote(lat.at[0, pl.ds(tok - r, r)], kbuf.at[k - 1, pl.ds(0, r)],
                      key_s.at[k - 1], key_r.at[k - 1], ctx=lax.rem(d + k, n))

    def id_copy(o):
        return remote(ids, idbuf.at[d], id_s.at[o - 1], id_r.at[o - 1], ctx=lax.rem(d + o, n))

    for k in range(1, reach):
        @pl.when(d + k < n)
        def _(k=k):
            key_copy(k).start()

    for o in range(1, n):
        id_copy(o).start()
    for k in range(1, reach):
        @pl.when(d - k < 0)
        def _(k=k):
            kbuf[k - 1] = jnp.zeros_like(kbuf[k - 1])
    idbuf[d] = ids[...]

    def repack(src, dst, width):
        group = 16 // qd

        def step(i, _):
            got = [
                src[0, :, pl.ds(pl.multiple_of((i * group + t) * width, 128), width)].astype(F32)
                for t in range(group)
            ]
            dst[pl.ds(pl.multiple_of(i * 16, 16), 16), :] = jnp.concatenate(got, axis=0).astype(BF)
            return 0

        lax.fori_loop(0, (HEADS // 2) // group, step, 0)

    copy_q.wait()
    repack(qraw, qs, pair)
    copy_g.wait()
    repack(graw, gs, 2 * LATENT)

    R = (HEADS // 2) * qd
    qrow = lax.broadcasted_iota(jnp.int32, (R, 1), 0) % qd
    own_ids = ids[...]
    qid = jnp.zeros((R, 1), jnp.int32)
    for i in range(qd):
        qid = jnp.where(qrow == i, own_ids[:, tok - qd + i:tok - qd + i + 1], qid)

    def query(par):
        return qs[:, 0:wide] if par == 0 else qs[:, pair - wide:pair]

    def grad(par):
        return gs[:, par * LATENT:(par + 1) * LATENT]

    def keys_of(k):
        return lat[0] if k == 0 else kbuf[k - 1, 0:rows_of[k], :]

    def block_products(k):
        kb = keys_of(k)
        zero = jnp.zeros((rows_of[k], pad), BF)
        padded = [jnp.concatenate([kb, zero], axis=1), jnp.concatenate([zero, kb], axis=1)]
        s = [dot(query(par), padded[par], ((1,), (1,))) for par in (0, 1)]
        dp = [dot(grad(par), kb[:, :LATENT], ((1,), (1,))) for par in (0, 1)]
        return s, dp

    products = [block_products(0)]

    for o in range(1, n):
        id_copy(o).wait_send()
        remote(ids, idbuf.at[lax.rem(d - o + n, n)], id_s.at[o - 1], id_r.at[o - 1],
               ctx=lax.rem(d + o, n)).wait_recv()
    for k in range(1, reach):
        @pl.when(d - k >= 0)
        def _(k=k):
            key_copy(k).wait_recv()
    for k in range(1, reach):
        products.append(block_products(k))

    allowed = []
    for k in range(reach):
        r = rows_of[k]
        row = own_ids if k == 0 else idbuf[jnp.maximum(d - k, 0)]
        row = row[:, tok - r:]
        lane = lax.broadcasted_iota(jnp.int32, (1, r), 1)
        ok = qid == row
        if k == 0:
            ok = ok & (lane <= tok - qd + qrow)
        else:
            reachable = jnp.where(lane + (tok - r) >= (k + 1) * tok - span, 1, 0)
            reachable = reachable * jnp.where(d - k >= 0, 1, 0)
            ok = ok & (reachable == 1)
        allowed.append(ok)

    dscores, probs = [[], []], [[], []]
    for par in (0, 1):
        s = [jnp.where(allowed[k], products[k][0][par] * score_scale, -1e30) for k in range(reach)]
        top = functools.reduce(jnp.maximum, [jnp.max(x, axis=1, keepdims=True) for x in s])
        w = [jnp.exp(x - top) for x in s]
        total = sum(jnp.sum(x, axis=1, keepdims=True) for x in w)
        w = [x / total for x in w]
        dps = [products[k][1][par] for k in range(reach)]
        rd = sum(jnp.sum(a * b, axis=1, keepdims=True) for a, b in zip(w, dps))
        for k in range(reach):
            dscores[par].append((w[k] * (dps[k] - rd) * score_scale).astype(BF))
            probs[par].append(w[k].astype(BF))

    def part_of(k):
        a = dot(dscores[0][k], query(0), ((0,), (0,)))[:, :kw]
        b = dot(dscores[1][k], query(1), ((0,), (0,)))[:, pad:pad + kw]
        v = dot(probs[0][k], grad(0), ((0,), (0,))) + dot(probs[1][k], grad(1), ((0,), (0,)))
        return (a + b + jnp.concatenate([v, jnp.zeros((rows_of[k], kw - LATENT), F32)], axis=1)).astype(BF)

    def part_copy(k, to):
        r = rows_of[k]
        return remote(psend.at[k - 1, pl.ds(0, r)], precv.at[k - 1, pl.ds(0, r)],
                      part_s.at[k - 1], part_r.at[k - 1], ctx=to)

    for k in range(1, reach):
        psend[k - 1, 0:rows_of[k], :] = part_of(k)

        @pl.when(d - k >= 0)
        def _(k=k):
            part_copy(k, jnp.maximum(d - k, 0)).start()

        @pl.when(d + k >= n)
        def _(k=k):
            precv[k - 1] = jnp.zeros_like(precv[k - 1])
    mine = part_of(0).astype(F32)

    eye = lax.broadcasted_iota(jnp.int32, (tok, tok), 0) == lax.broadcasted_iota(jnp.int32, (tok, tok), 1)
    doc_lane = lax.broadcasted_iota(jnp.int32, (1, 128), 1)
    member = []
    for j in range(n):
        col = jnp.sum(jnp.where(eye, idbuf[j], 0).astype(F32), axis=1, keepdims=True)
        member.append(jnp.where(col == doc_lane.astype(F32), 1.0, 0.0))

    for k in range(1, reach):
        @pl.when(d + k < n)
        def _(k=k):
            part_copy(k, jnp.maximum(d - k, 0)).wait_recv()
    for k in range(1, reach):
        r = rows_of[k]
        got = precv[k - 1, 0:r, :].astype(F32)
        if r < tok:
            got = jnp.concatenate([jnp.zeros((tok - r, kw), F32), got], axis=0)
        mine = mine + got
    mine_low = mine.astype(BF)
    full[d] = mine_low

    piece = tok // pieces

    def relay(direction, s, p):
        ss, rs = (up_s, up_r) if direction > 0 else (dn_s, dn_r)
        block = jnp.clip(d - direction * s, 0, n - 1)
        ref = full.at[block, pl.ds(p * piece, piece)]
        return remote(ref, ref, ss.at[s, p], rs.at[s, p], ctx=jnp.clip(d + direction, 0, n - 1))

    def arriving(direction, s, p):
        ss, rs = (up_s, up_r) if direction > 0 else (dn_s, dn_r)
        block = jnp.clip(d - direction * (s + 1), 0, n - 1)
        ref = full.at[block, pl.ds(p * piece, piece)]
        return remote(ref, ref, ss.at[s, p], rs.at[s, p], ctx=jnp.clip(d + direction, 0, n - 1))

    def can_send(direction, s):
        if direction > 0:
            return (d - s >= 0) & (d + 1 < n)
        return (d + s < n) & (d - 1 >= 0)

    def will_get(direction, s):
        return d - s - 1 >= 0 if direction > 0 else d + s + 1 < n

    for p in range(pieces):
        for direction in (1, -1):
            @pl.when(can_send(direction, 0))
            def _(p=p, direction=direction):
                relay(direction, 0, p).start()
    padded_out = jnp.concatenate([mine_low.astype(F32), jnp.zeros((tok, pad), F32)], axis=1)
    gk_out[0] = jnp.transpose(padded_out)[:kw].astype(BF)
    for s in range(n - 1):
        for p in range(pieces):
            for direction in (1, -1):
                @pl.when(will_get(direction, s))
                def _(p=p, s=s, direction=direction):
                    arriving(direction, s, p).wait_recv()
                if s + 1 < n - 1:
                    @pl.when(can_send(direction, s + 1))
                    def _(p=p, s=s, direction=direction):
                        relay(direction, s + 1, p).start()

    norms = jnp.zeros((1, 128), F32)
    for j in range(n):
        v = full[j].astype(F32)
        norms = norms + jnp.sum(member[j] * jnp.sum(v * v, axis=1, keepdims=True), axis=0, keepdims=True)
    limits = lim[...]
    if ndocs < 128:
        limits = jnp.concatenate([limits, jnp.zeros((1, 128 - ndocs), F32)], axis=1)
    factor = jnp.minimum(1.0, limits / jnp.sqrt(norms + norm_eps))
    for j in range(n):
        f = jnp.sum(member[j] * factor, axis=1, keepdims=True)
        scaled = (full[j].astype(F32) * f).astype(BF).astype(F32)
        scaled = jnp.concatenate([scaled, jnp.zeros((tok, pad), F32)], axis=1)
        turned = jnp.transpose(scaled)
        scT[:, j * tok:(j + 1) * tok] = turned[:kw].astype(BF)

    copy_h.wait()
    w_out[...] = dot(scT[...], hid[0], ((1,), (0,)))

    for k in range(1, reach):
        @pl.when(d + k < n)
        def _(k=k):
            key_copy(k).wait_send()

        @pl.when(d - k >= 0)
        def _(k=k):
            part_copy(k, jnp.maximum(d - k, 0)).wait_send()
    for s in range(n - 1):
        for p in range(pieces):
            for direction in (1, -1):
                @pl.when(can_send(direction, s))
                def _(p=p, s=s, direction=direction):
                    relay(direction, s, p).wait_send()


def flush(gk, w, gk_out, w_out, sem):
    a = pltpu.make_async_copy(gk, gk_out, sem.at[0])
    b = pltpu.make_async_copy(w, w_out, sem.at[1])
    a.start()
    b.start()
    a.wait()
    b.wait()


def pair_body(cfg, *refs):
    n = cfg["n"]
    tok = cfg["tok"]
    kw = cfg["kw"]
    qd = cfg["qd"]
    halo = cfg["halo"]
    ndocs = cfg["ndocs"]
    splits = cfg["splits"]
    seq = n * tok
    wide = -(-kw // 128) * 128
    pad = wide - kw
    share = kw // 8
    np_ = len(splits)
    offs = [sum(splits[:p]) for p in range(np_)]
    (lat_hbm, ids_hbm, lim_hbm, q_hbm, g_hbm, h_hbm, gk_dst, w_dst,
     gk_out, w_out, lat_t, lat, ids, lim, qraw, graw, hid, qs, gs, kbuf, krot, kgot, lath, hkey, idbuf,
     psend, precv, hsend, hrecv, ownb, own2, full, gkr, nbuf, lhs,
     loc, out_s, key_r, hid_r, part_r, halo_r, own_r, gk_r, nrm_r, blk_r, rs_r) = refs[:46]
    tail = refs[46:]
    d = lax.axis_index("ctx")
    m = lax.axis_index("grp")
    c = lax.rem(m, 2)
    xb = lax.rem(m // 2, 2)
    yb = lax.rem(m // 4, 2)
    base = m - c
    mate = base + 1 - c
    flip_x = m + 2 - 4 * xb
    flip_y = m + 4 - 8 * yb
    flip_xy = flip_x + flip_y - m
    cols = w_out.shape[1]
    wing = cols // 2

    def remote(src, dst, ss, rs, **where):
        return pltpu.make_async_remote_copy(
            src_ref=src, dst_ref=dst, send_sem=ss, recv_sem=rs,
            device_id=where, device_id_type=pl.DeviceIdType.MESH,
        )

    def drain(ref, sem):
        pltpu.make_async_copy(ref, ref, sem).wait()

    loads = [
        pltpu.make_async_copy(lat_hbm, lat_t, loc.at[0]),
        pltpu.make_async_copy(ids_hbm, ids, loc.at[1]),
        pltpu.make_async_copy(q_hbm, qraw, loc.at[2]),
        pltpu.make_async_copy(g_hbm, graw, loc.at[3]),
        pltpu.make_async_copy(lim_hbm, lim, loc.at[4]),
        pltpu.make_async_copy(h_hbm.at[0], hid.at[c], loc.at[5]),
    ]
    for copy in loads:
        copy.start()

    barrier = pltpu.get_barrier_semaphore()

    def greet(**where):
        pl.semaphore_signal(barrier, inc=1, device_id=where, device_id_type=pl.DeviceIdType.MESH)

    close = 0
    for o in (-2, 2, -1, 1):
        there = (d + o >= 0) & (d + o < n)
        close = close + jnp.where(there, 2, 0)

        @pl.when(there)
        def _(o=o):
            for who in (m, mate):
                greet(ctx=jnp.clip(d + o, 0, n - 1), grp=who)
    greet(grp=mate)
    greet(grp=flip_x)
    greet(grp=flip_y)
    greet(grp=flip_xy)

    loads[0].wait()
    keys_t = jnp.concatenate([lat_t[0].astype(F32), jnp.zeros((pad, tok), F32)], axis=0)
    keys = jnp.transpose(keys_t)
    lat[...] = keys.astype(BF)
    near = tok // 2
    rope = kw - LATENT
    krot[...] = jnp.concatenate([keys[:near, LATENT:kw], keys[near:, LATENT:kw]], axis=1).astype(BF)
    lath[...] = keys[tok - halo:].astype(BF)
    loads[1].wait()
    pl.semaphore_wait(barrier, close + 4)

    def id_copy(k):
        return remote(ids, idbuf.at[k - 1], out_s.at[12 + k], key_r.at[k - 1], ctx=lax.rem(d + k, n))

    def key_copy(k):
        if k == 1:
            return [
                remote(lat.at[:, pl.ds(0, LATENT)], kbuf.at[pl.ds(0, tok), pl.ds(0, LATENT)],
                       out_s.at[15], key_r.at[2], ctx=lax.rem(d + 1, n)),
                remote(krot, kgot, out_s.at[16], key_r.at[3], ctx=lax.rem(d + 1, n)),
            ]
        return [remote(lath, hkey, out_s.at[17], key_r.at[4], ctx=lax.rem(d + 2, n))]

    for k in (2, 1):
        @pl.when(d + k < n)
        def _(k=k):
            id_copy(k).start()
            for copy in key_copy(k):
                copy.start()

    hid_copy = remote(h_hbm.at[0], hid.at[c], out_s.at[0], hid_r.at[0], grp=mate)
    hid_copy.start()

    @pl.when(d < 1)
    def _():
        kbuf[0:tok, :] = jnp.zeros((tok, wide), BF)
        kgot[...] = jnp.zeros_like(kgot)
        idbuf[0] = jnp.zeros_like(idbuf[0])

    @pl.when(d < 2)
    def _():
        hkey[...] = jnp.zeros_like(hkey)
        idbuf[1] = jnp.zeros_like(idbuf[1])

    group = 16 // qd
    R = (HEADS // 2) * qd

    def repack(src, dst, width):
        def step(i, _):
            got = [
                src[0, :, pl.ds(pl.multiple_of((i * group + t) * 2 * width, 128), 2 * width)].astype(F32)
                for t in range(group)
            ]
            got = jnp.concatenate(got, axis=0)
            for par in (0, 1):
                one = got[:, par * width:(par + 1) * width]
                if width % 128:
                    one = jnp.concatenate([one, jnp.zeros((16, pad), F32)], axis=1)
                dst[pl.ds(pl.multiple_of(par * R + i * 16, 16), 16), :] = one.astype(BF)
            return 0

        lax.fori_loop(0, (HEADS // 2) // group, step, 0)

    loads[2].wait()
    repack(qraw, qs, kw)
    loads[3].wait()
    repack(graw, gs, LATENT)

    def turn_ids(row):
        return jnp.transpose(jnp.broadcast_to(row.astype(F32), (tok, tok)))

    def across(x):
        return jnp.concatenate([x] * (2 * R // tok), axis=1)

    qrow = lax.broadcasted_iota(jnp.int32, (1, tok), 1) % qd
    own_ids = ids[...]
    qid = jnp.zeros((1, tok), F32)
    for i in range(qd):
        qid = jnp.where(qrow == i, own_ids[:, tok - qd + i:tok - qd + i + 1].astype(F32), qid)

    def block_products(keys):
        return (dot(keys, qs[...], ((1,), (1,))), dot(keys[:, :LATENT], gs[...], ((1,), (1,))))

    key_row = lax.broadcasted_iota(jnp.int32, (tok, tok), 0)
    s0, dp0 = block_products(lat[...])
    ok0 = jnp.where(turn_ids(own_ids) == qid, 1, 0) * jnp.where(key_row <= tok - qd + qrow, 1, 0)
    s0 = jnp.where(across(ok0) == 1, s0 * score_scale, -1e30)
    top0 = jnp.max(s0, axis=0, keepdims=True)

    for k in (2, 1):
        @pl.when(d >= k)
        def _(k=k):
            id_copy(k).wait_recv()
            for copy in key_copy(k):
                copy.wait_recv()
    got = kgot[...].astype(F32)
    got = jnp.concatenate([got[:, :rope], got[:, rope:]], axis=0)
    kbuf[0:tok, LATENT:wide] = jnp.concatenate([got, jnp.zeros((tok, wide - kw), F32)], axis=1).astype(BF)
    kbuf[tok:tok + 16, :] = jnp.concatenate([jnp.zeros((16 - halo, wide), F32), hkey[...].astype(F32)], axis=0).astype(BF)
    s1, dp1 = block_products(kbuf[...])
    ok1 = jnp.where(turn_ids(idbuf[0]) == qid, 1, 0)
    ok1 = ok1 * jnp.where(key_row >= 2 * tok - cfg["span"], 1, 0) * jnp.where(d >= 1, 1, 0)
    ok2 = jnp.where(turn_ids(idbuf[1]) == qid, 1, 0)
    ok2 = ok2 * jnp.where(key_row >= 3 * tok - cfg["span"], 1, 0) * jnp.where(d >= 2, 1, 0)
    ok1 = jnp.concatenate([ok1, ok2[tok - 16:]], axis=0)
    s1 = jnp.where(across(ok1) == 1, s1 * score_scale, -1e30)
    top = jnp.maximum(top0, jnp.max(s1, axis=0, keepdims=True))
    w0, w1 = jnp.exp(s0 - top), jnp.exp(s1 - top)
    scale = 1.0 / (jnp.sum(w0, axis=0, keepdims=True) + jnp.sum(w1, axis=0, keepdims=True))
    w0, w1 = w0 * scale, w1 * scale
    rd = jnp.sum(w0 * dp0, axis=0, keepdims=True) + jnp.sum(w1 * dp1, axis=0, keepdims=True)

    def part_of(w, dp):
        a = dot((w * (dp - rd) * score_scale).astype(BF), qs[...], ((1,), (0,)))
        v = dot(w.astype(BF), gs[...], ((1,), (0,)))
        return a + jnp.concatenate([v, jnp.zeros((v.shape[0], wide - LATENT), F32)], axis=1)

    def halves(turned):
        out = []
        for h in (0, 1):
            rows = []
            for p in range(np_):
                for q in range(4):
                    start = share * (2 * q + h) + offs[p]
                    rows.append(turned[start:start + splits[p]])
            out.append(jnp.concatenate(rows, axis=0))
        return out

    def halo_copy(h):
        return remote(hsend, hrecv.at[c], out_s.at[2], halo_r.at[0],
                      ctx=jnp.maximum(d - 2, 0), grp=base + h)

    def part_copy(h, p):
        rows = pl.ds(4 * offs[p], 4 * splits[p])
        return remote(psend.at[h, rows], precv.at[c, rows], out_s.at[1], part_r.at[p],
                      ctx=jnp.maximum(d - 1, 0), grp=base + h)

    part1 = part_of(w1, dp1)
    hsend[...] = part1[tok + 16 - halo:].astype(BF)

    @pl.when(d >= 2)
    def _():
        for h in (0, 1):
            halo_copy(h).start()

    turned = halves(jnp.transpose(part1[:tok]))
    for h in (0, 1):
        psend[h] = turned[h].astype(BF)

    @pl.when(d >= 1)
    def _():
        for p in range(np_):
            for h in (0, 1):
                part_copy(h, p).start()

    @pl.when(d + 1 >= n)
    def _():
        precv[...] = jnp.zeros_like(precv)

    @pl.when(d + 2 >= n)
    def _():
        hrecv[...] = jnp.zeros_like(hrecv)

    turned = halves(jnp.transpose(part_of(w0, dp0)))
    for h in (0, 1):
        ownb[h] = turned[h].astype(BF)
    own_copy = remote(ownb.at[1 - c], own2.at[c], out_s.at[3], own_r.at[0], grp=mate)
    own_copy.start()
    own2[c] = ownb[c]
    own_copy.wait_recv()

    def rows_at(p):
        return pl.ds(8 * offs[p], 8 * splits[p])

    steps = (-1, 1, -2, 2)

    def slot(o, source):
        if o in (-1, 1):
            return 1
        return jnp.where(source == (n - 1 if o < 0 else 0), 0, 1)

    def spread(o, p):
        ref = full.at[d, rows_at(p)]
        return remote(ref, ref, out_s.at[7 + steps.index(o)], blk_r.at[slot(o, d), p], ctx=jnp.clip(d + o, 0, n - 1))

    def spread_from(o, p):
        ref = full.at[jnp.clip(d - o, 0, n - 1), rows_at(p)]
        return remote(ref, ref, out_s.at[7 + steps.index(o)], blk_r.at[slot(o, d - o), p], ctx=jnp.clip(d - o, 0, n - 1))

    def pass_end(o, p):
        ref = full.at[n - 1 if o < 0 else 0, rows_at(p)]
        return remote(ref, ref, out_s.at[11 if o < 0 else 12], blk_r.at[1, p], ctx=jnp.clip(d + o, 0, n - 1))

    def reaches(o):
        return (d + o >= 0) & (d + o < n)

    def passes(o):
        return d == (1 if o < 0 else n - 2)

    def ends(o):
        return d == (0 if o < 0 else n - 1)

    @pl.when(d + 2 < n)
    def _():
        drain(hrecv, halo_r.at[0])

    side = []
    for g in (0, 1):
        block = jnp.concatenate([jnp.zeros((tok - halo, wide), F32), hrecv[g].astype(F32)], axis=0)
        turned = halves(jnp.transpose(block))
        side.append(jnp.where(c == 0, turned[0], turned[1]))

    def spread_all(p):
        for o in steps:
            @pl.when(reaches(o))
            def _(o=o):
                spread(o, p).start()

    token_norm = [jnp.zeros((1, tok), F32) for _ in (0, 1)]
    for p in range(np_):
        @pl.when(d + 1 < n)
        def _(p=p):
            drain(precv.at[:, pl.ds(4 * offs[p], 4 * splits[p])], part_r.at[p])
        lo, size = 4 * offs[p], 4 * splits[p]
        for g in (0, 1):
            value = own2[g, lo:lo + size].astype(F32) + precv[g, lo:lo + size].astype(F32)
            value = (value + side[g][lo:lo + size]).astype(BF)
            full[d, 2 * lo + g * size:2 * lo + (g + 1) * size] = value
            value = value.astype(F32)
            token_norm[g] = token_norm[g] + jnp.sum(value * value, axis=0, keepdims=True)
        if p == 0:
            spread_all(p)

    loads[4].wait()
    limits = jnp.concatenate([lim[...], jnp.zeros((1, tok - ndocs), F32)], axis=1)
    nbuf[c, d] = jnp.concatenate(
        token_norm + [own_ids.astype(F32), limits, jnp.zeros((4, tok), F32)], axis=0)

    def norm_copy(o, flip):
        ref = nbuf.at[c, d]
        return remote(ref, ref, out_s.at[5 + flip], nrm_r.at[flip], ctx=lax.rem(d + o, n), grp=mate if flip else m)

    peers = [(o, flip) for o in range(n) for flip in (0, 1) if o or flip]
    for o, flip in peers:
        norm_copy(o, flip).start()
    spread_all(1)

    def spread_rest(p):
        if p < np_:
            @pl.when(ends(-1) | ends(1))
            def _():
                spread_all(p)

    def spread_mid(p):
        if p < np_:
            @pl.when(jnp.logical_not(ends(-1) | ends(1)))
            def _():
                spread_all(p)

    for p in range(2, np_):
        spread_rest(p)

    def gk_copy(p):
        lo, size = 4 * offs[p], 4 * splits[p]
        src = full.at[d, pl.ds(pl.multiple_of(2 * lo + (1 - c) * size, 16), size)]
        return remote(src, gkr.at[pl.ds(lo, size)], out_s.at[4], gk_r.at[0], grp=mate)

    for p in range(np_):
        gk_copy(p).start()

    factors = []

    def make_factors():
        drain(nbuf.at[0, pl.ds(0, n - 1)], nrm_r.at[0])
        drain(nbuf.at[0], nrm_r.at[1])
        rows = -(-ndocs // 8) * 8
        sub = lax.broadcasted_iota(jnp.int32, (rows, tok), 0).astype(F32)
        lane = lax.broadcasted_iota(jnp.int32, (rows, tok), 1).astype(F32)
        for g in (0, 1):
            member = [jnp.where(nbuf[g, b, 2:3] == sub, 1.0, 0.0) for b in range(n)]
            norms = sum(
                jnp.sum(member[b] * (nbuf[0, b, g:g + 1] + nbuf[1, b, g:g + 1]), axis=1, keepdims=True)
                for b in range(n))
            top = jnp.sum(jnp.where(lane == sub, nbuf[g, 0, 3:4], 0.0), axis=1, keepdims=True)
            factor = jnp.minimum(1.0, top / jnp.sqrt(norms + norm_eps))
            factors.append([jnp.sum(member[b] * factor, axis=0, keepdims=True) for b in range(n)])

    def forward(p):
        for o in (-1, 1):
            @pl.when(passes(o))
            def _(o=o):
                spread_from(2 * o, p).wait_recv()
                pass_end(o, p).start()
        if p:
            spread_mid(p + 1)

    def gather(p):
        @pl.when(ends(-1) | ends(1))
        def _():
            drain(full.at[pl.ds(0, n - 1), rows_at(p)], blk_r.at[1, p])

        @pl.when(jnp.logical_not(ends(-1) | ends(1)))
        def _():
            drain(full.at[pl.ds(0, n - 2), rows_at(p)], blk_r.at[1, p])

    straight = cfg["straight"]
    bufs, pos = [], 0
    for p in range(np_):
        if p in straight:
            bufs.append(tail[pos:pos + 3])
            pos += 3
        else:
            bufs.append(tail[pos:pos + 3])
            pos += 3

    def direct(p, j):
        out, back, _ = bufs[p]
        return remote(out.at[j], back.at[j], out_s.at[18 + p], rs_r.at[p, 0, 0],
                      grp=(flip_x, flip_y, flip_xy)[j])

    def hop(p, w, stage):
        out, back, _ = bufs[p]
        where = (flip_x, flip_y) if w == 0 else (flip_y, flip_x)
        part = pl.ds(0, 2) if stage == 0 else pl.ds(2, 1)
        src, dst = out.at[w, part], back.at[w, part]
        return remote(src, dst, out_s.at[18 + p], rs_r.at[p, w, stage], grp=where[stage])

    bits = ((xb, yb), (yb, xb))

    def chip(w, moving, other):
        return other * 2 + moving if w == 0 else moving * 2 + other

    def wing_of(p, w):
        lo, size = 4 * offs[p], 4 * splits[p]
        return sum(
            dot(lhs[lo:lo + size, g * seq:(g + 1) * seq], hid[g, :, w * wing:(w + 1) * wing], ((1,), (0,)))
            for g in (0, 1))

    def product(p):
        lo, size = 4 * offs[p], 4 * splits[p]
        for g in (0, 1):
            for b in range(n):
                value = full[b, 2 * lo + g * size:2 * lo + (g + 1) * size].astype(F32)
                at = (g * n + b) * tok
                lhs[lo:lo + size, at:at + tok] = (value * factors[g][b]).astype(BF)
        if p in straight:
            first, _, total = bufs[p]
            for w in (0, 1):
                cut = slice(w * wing, (w + 1) * wing)
                total[:, :, cut] = wing_of(p, w).reshape(4, splits[p], wing)
            for j, q in ((2, 2 * (1 - yb) + 1 - xb), (0, 2 * yb + 1 - xb), (1, 2 * (1 - yb) + xb)):
                first[j] = total[q].astype(BF)
                direct(p, j).start()
            return
        for w in (0, 1):
            first, _, total = bufs[p]
            total[w] = wing_of(p, w).reshape(total.shape[1:])
            for o in (0, 1):
                first[w, o] = total[w, chip(w, 1 - bits[w][0], o)].astype(BF)
            hop(p, w, 0).start()

    def pass_on(p):
        for w in (0, 1):
            second, back, total = bufs[p]
            hop(p, w, 0).wait_recv()
            second[w, 2] = (total[w, chip(w, bits[w][0], 1 - bits[w][1])] + back[w, 1 - bits[w][1]].astype(F32)).astype(BF)
            hop(p, w, 1).start()

    def put(p):
        rows = pl.ds(offs[p], splits[p])
        return pltpu.make_async_copy(w_out.at[rows], w_dst.at[rows], loc.at[7])

    put_keys = pltpu.make_async_copy(gk_out, gk_dst, loc.at[6])

    def finish(p):
        last(p)
        put(p).start()

    def last(p):
        if p in straight:
            _, back, total = bufs[p]
            value = total[2 * yb + xb]
            drain(back, rs_r.at[p, 0, 0])
            for j in range(3):
                value = value + back[j].astype(F32)
            w_out[offs[p]:offs[p] + splits[p], :] = value
            return
        for w in (0, 1):
            _, back, total = bufs[p]
            kept = total[w, chip(w, bits[w][0], bits[w][1])] + back[w, bits[w][1]].astype(F32)
            hop(p, w, 1).wait_recv()
            w_out[offs[p]:offs[p] + splits[p], w * wing:(w + 1) * wing] = kept + back[w, 2].astype(F32)

    def write_keys():
        drain(gkr, gk_r.at[0])
        order = [None] * (8 * np_)
        for p in range(np_):
            lo, size = 4 * offs[p], splits[p]
            near = [full[d, 2 * lo + g * 4 * size:2 * lo + (g + 1) * 4 * size].astype(F32) for g in (0, 1)]
            near = jnp.where(c == 0, near[0], near[1])
            far = gkr[lo:lo + 4 * size].astype(F32)
            for h in (0, 1):
                value = jnp.where(c == h, near, far)
                for q in range(4):
                    order[(2 * q + h) * np_ + p] = value[q * size:(q + 1) * size]
        gk_out[0] = jnp.concatenate(order, axis=0).astype(BF)
        put_keys.start()

    forward(0)
    forward(1)
    make_factors()
    loads[5].wait()
    hid_copy.wait_recv()
    staged = [p for p in range(np_) if p not in straight]
    moved, done = [], []
    for p in range(np_):
        gather(p)
        product(p)
        if p + 2 < np_:
            forward(p + 2)
        if p == 0:
            write_keys()
        for q in staged:
            if q + cfg["lag"] == p:
                pass_on(q)
                moved.append(q)
            if q + 2 * cfg["lag"] == p:
                finish(q)
                done.append(q)
    for q in staged:
        if q not in moved:
            pass_on(q)
    for q in range(np_):
        if q not in done:
            finish(q)
    put_keys.wait()
    drain(w_out, loc.at[7])

    for k in (1, 2):
        @pl.when(d + k < n)
        def _(k=k):
            id_copy(k).wait_send()
            for copy in key_copy(k):
                copy.wait_send()
    hid_copy.wait_send()

    @pl.when(d >= 2)
    def _():
        drain(hrecv, out_s.at[2])

    @pl.when(d >= 1)
    def _():
        drain(psend, out_s.at[1])
    own_copy.wait_send()
    drain(gkr, out_s.at[4])
    drain(nbuf.at[0, pl.ds(0, n - 1)], out_s.at[5])
    drain(nbuf.at[0], out_s.at[6])
    for i, o in enumerate(steps):
        @pl.when(reaches(o))
        def _(i=i):
            drain(full.at[0], out_s.at[7 + i])
    for i, o in enumerate((-1, 1)):
        @pl.when(passes(o))
        def _(i=i):
            drain(full.at[0], out_s.at[11 + i])
    for p in range(np_):
        drain(bufs[p][0], out_s.at[18 + p])


def pair_scratch(cfg, latent, queries, out_grad, hidden, clip_limits):
    n, tok, kw, halo = cfg["n"], cfg["tok"], cfg["kw"], cfg["halo"]
    splits = cfg["splits"]
    np_ = len(splits)
    half = kw // 2
    wide = -(-kw // 128) * 128
    rows = (HEADS // 2) * cfg["qd"]
    cols = hidden.shape[2]
    seq = n * tok
    dma = pltpu.SemaphoreType.DMA
    v = pltpu.VMEM
    scratch = [
        v((1, kw, tok), BF), v((kw // 8, cols), F32),
        v((1, kw, tok), BF), v((tok, wide), BF), v((1, tok), jnp.int32), v(clip_limits.shape, F32),
        v(queries.shape, BF), v(out_grad.shape, BF), v((2, seq, cols), BF),
        v((2 * rows, wide), BF), v((2 * rows, LATENT), BF),
        v((tok + 16, wide), BF), v((tok // 2, 2 * (kw - LATENT)), BF), v((tok // 2, 2 * (kw - LATENT)), BF),
        v((halo, wide), BF), v((halo, wide), BF), v((2, 1, tok), jnp.int32),
        v((2, half, tok), BF), v((2, half, tok), BF), v((halo, wide), BF), v((2, halo, wide), BF),
        v((2, half, tok), BF), v((2, half, tok), BF), v((n, kw, tok), BF), v((half, tok), BF),
        v((2, n, 8, tok), F32), v((half, 2 * seq), BF),
        dma((8,)), dma((18 + np_,)), dma((5,)), dma((1,)), dma((np_,)), dma((1,)), dma((1,)), dma((1,)), dma((2,)),
        dma((2, np_)), dma((np_, 2, 2)),
    ]
    for p, size in enumerate(splits):
        if p in cfg["straight"]:
            scratch += [v((3, size, cols), BF), v((3, size, cols), BF), v((4, size, cols), F32)]
            continue
        scratch += [
            v((2, 3, size, cols // 2), BF), v((2, 3, size, cols // 2), BF), v((2, 4, size, cols // 2), F32),
        ]
    return scratch


def row_splits(share):
    units = share // 8
    cuts = [0] + [units * p // 9 for p in (3, 6)] + [units]
    return tuple(8 * (b - a) for a, b in zip(cuts, cuts[1:]) if b > a)


def pair_call(cfg, latent, queries, out_grad, hidden, doc_ids, clip_limits):
    anywhere = pl.BlockSpec(memory_space=pl.ANY)
    tok, kw = cfg["tok"], cfg["kw"]
    grad_keys, weight = pl.pallas_call(
        functools.partial(pair_body, cfg),
        out_shape=(
            pltpu.VMEM((1, kw, tok), BF),
            pltpu.VMEM((kw // 8, hidden.shape[2]), F32),
        ),
        in_specs=[anywhere] * 6,
        out_specs=(anywhere, anywhere),
        scratch_shapes=pair_scratch(cfg, latent, queries, out_grad, hidden, clip_limits),
        compiler_params=pltpu.CompilerParams(
            collective_id=0, has_side_effects=True, vmem_limit_bytes=56 * 1024 * 1024),
    )(jnp.swapaxes(latent, 1, 2), doc_ids, clip_limits, queries, out_grad, hidden)
    return (jnp.swapaxes(grad_keys, 1, 2), weight)


def on_device(latent, queries, out_grad, hidden, doc_ids, clip_limits):
    n = lax.axis_size("ctx")
    groups = lax.axis_size("grp")
    tok, kw = latent.shape[1:]
    qd = queries.shape[1]
    seq = tok * n
    span = seq // 2 + qd
    reach = min(n, -(-span // tok))
    cols = hidden.shape[2]
    last = min(tok, -(-(span - (reach - 1) * tok) // 16) * 16)
    rows_of = [tok] * (reach - 1) + [last]
    ndocs = clip_limits.shape[1]
    share = kw // 8
    paired = (groups == 8 and n == 4 and reach == 3 and last <= tok and cols % 256 == 0 and kw % 64 == 0
              and tok % 128 == 0 and ndocs <= tok and span <= 2 * tok + 16 and 2 * (kw - LATENT) == 128)
    if paired:
        cfg = dict(n=n, tok=tok, kw=kw, qd=qd, halo=-(-(span - 2 * tok) // 4) * 4, span=span, ndocs=ndocs, splits=row_splits(share), straight=(0,), lag=1)
        return pair_call(cfg, latent, queries, out_grad, hidden, doc_ids, clip_limits)
    pieces = 2
    cfg = dict(n=n, tok=tok, kw=kw, qd=qd, reach=reach, rows_of=rows_of, span=span, ndocs=ndocs,
               pieces=pieces)
    rows = (HEADS // 2) * qd
    dma = pltpu.SemaphoreType.DMA
    scratch = [
        pltpu.VMEM(queries.shape, BF),
        pltpu.VMEM(out_grad.shape, BF),
        pltpu.VMEM(hidden.shape, BF),
        pltpu.VMEM((rows, 2 * kw), BF),
        pltpu.VMEM((rows, 2 * LATENT), BF),
        pltpu.VMEM((reach - 1, tok, kw), BF),
        pltpu.VMEM((n, 1, tok), jnp.int32),
        pltpu.VMEM((reach - 1, tok, kw), BF),
        pltpu.VMEM((reach - 1, tok, kw), BF),
        pltpu.VMEM((n, tok, kw), BF),
        pltpu.VMEM((kw, seq), BF),
        dma((3,)),
        dma((reach - 1,)), dma((reach - 1,)),
        dma((n - 1,)), dma((n - 1,)),
        dma((reach - 1,)), dma((reach - 1,)),
        dma((n - 1, pieces)), dma((n - 1, pieces)),
        dma((n - 1, pieces)), dma((n - 1, pieces)),
        pltpu.VMEM((1, tok, kw), BF),
    ]
    vmem = pl.BlockSpec(memory_space=pltpu.VMEM)
    anywhere = pl.BlockSpec(memory_space=pl.ANY)
    grad_keys, weight = pl.pallas_call(
        functools.partial(body, cfg),
        out_shape=(
            jax.ShapeDtypeStruct((1, kw, tok), BF),
            jax.ShapeDtypeStruct((kw, cols), F32),
        ),
        in_specs=[vmem, vmem, vmem, anywhere, anywhere, anywhere],
        out_specs=(vmem, vmem),
        scratch_shapes=scratch,
        compiler_params=pltpu.CompilerParams(
            collective_id=0, has_side_effects=True, vmem_limit_bytes=60 * 1024 * 1024),
    )(jnp.swapaxes(latent, 1, 2), doc_ids, clip_limits, queries, out_grad, hidden)
    weight = lax.psum_scatter(weight, "grp", scatter_dimension=0, tiled=True)
    return (jnp.swapaxes(grad_keys, 1, 2), weight)


def solution(mesh):
    return jax.shard_map(
        on_device,
        mesh=mesh,
        in_specs=(
            P("grp", "ctx", None),
            P("grp", "ctx", None),
            P("grp", "ctx", None),
            P("grp", None, "ctx"),
            P("grp", "ctx"),
            P("grp", None),
        ),
        out_specs=(P("grp", "ctx", None), P("grp", "ctx")),
        check_vma=False,
    )
```
